128 devices in a mesh: col: 2 (over core), row: 64 (over z, y, x).
Axes of the slice: x: 4, y: 4, z: 4, core: 2. Of those that a mesh axis runs over, the one named last changes fastest.
Arguments:
- hyper_params: float32 [3], replicated
- w_in: float32 [1, 1024, 65536], P(None, 'row', 'col')
- x_in: bfloat16 [1, 1024, 1024], P(None, None, 'row')
- dy_in: bfloat16 [1, 1024, 65536], P(None, None, 'col')
- row_in: float32 [1, 1024], P(None, 'row')
- col_in: float32 [1, 65536], P(None, 'col')
- w_out: float32 [1, 65536, 1024], P(None, 'col', 'row')
- x_out: bfloat16 [1, 1024, 65536], P(None, None, 'col')
- dy_out: bfloat16 [1, 1024, 1024], P(None, None, 'row')
- row_out: float32 [1, 65536], P(None, 'col')
- col_out: float32 [1, 1024], P(None, 'row')
Outputs:
- output 1: float32 [1, 1024, 65536], P(None, 'row', 'col')
- output 2: float32 [1, 1024], P(None, 'row')
- output 3: float32 [1, 65536], P(None, 'col')
- output 4: float32 [1, 65536, 1024], P(None, 'col', 'row')
- output 5: float32 [1, 65536], P(None, 'col')
- output 6: float32 [1, 1024], P(None, 'row')
All inputs are finite; a program needn't handle non-finite values.
Results may differ from the reference program's by a relative error of at most 0.001.
Values are sent between devices in bfloat16 or wider.
A program may use at most 1 GiB of HBM per device.

```python
import jax
import jax.numpy as jnp
from jax import lax

LAYERS = 1
TOKENS = 1024
D_MODEL = 1024
D_FF = 65536
LATENT_RANK = 4
EPS_ONE = 1e-30
EPS_TWO = 1e-3
TWO_PI = 6.283185307179586


def profile(draw_key, length):
    phase_off = jax.random.uniform(draw_key, (LAYERS, LATENT_RANK, 1), jnp.float32) * TWO_PI
    freq_rank = (jnp.arange(LATENT_RANK) + 1).astype(jnp.float32)[None, :, None]
    position = (jnp.arange(length).astype(jnp.float32) / length)[None, None, :]
    return 1.0 + 0.9 * jnp.sin(TWO_PI * freq_rank * position + phase_off)


def draw_matrix(draw_key, n_rows, n_cols):
    sub_keys = jax.random.split(draw_key, 10)
    latent = jax.random.normal(sub_keys[0], (LAYERS, TOKENS, LATENT_RANK), jnp.float32)
    load_rows = jax.random.normal(sub_keys[1], (LAYERS, LATENT_RANK, n_rows), jnp.float32) * profile(sub_keys[2], n_rows)
    load_cols = jax.random.normal(sub_keys[3], (LAYERS, LATENT_RANK, n_cols), jnp.float32) * profile(sub_keys[4], n_cols)
    x_act = jnp.einsum('ltk,lkm->ltm', latent, load_rows) + jax.random.normal(sub_keys[5], (LAYERS, TOKENS, n_rows), jnp.float32)
    dy_act = (jnp.einsum('ltk,lkn->ltn', latent, load_cols) + jax.random.normal(sub_keys[6], (LAYERS, TOKENS, n_cols), jnp.float32)) / TOKENS
    w_mat = jax.random.normal(sub_keys[7], (LAYERS, n_rows, n_cols), jnp.float32) * n_rows ** -0.5
    row_stat = 6.0 * jnp.exp(0.5 * jax.random.normal(sub_keys[8], (LAYERS, n_rows), jnp.float32))
    col_stat = 6.0 * jnp.exp(0.5 * jax.random.normal(sub_keys[9], (LAYERS, n_cols), jnp.float32))
    return w_mat, x_act.astype(jnp.bfloat16), dy_act.astype(jnp.bfloat16), row_stat, col_stat


def setup_inputs(seed: int = 0) -> dict:
    sub_keys = jax.random.split(jax.random.key(seed), 3)
    low_end = jnp.array([0.5, 0.5, 0.2], dtype=jnp.float32)
    span_width = jnp.array([0.3, 0.5, 0.2], dtype=jnp.float32)
    hyper_params = low_end + span_width * jax.random.uniform(sub_keys[0], (3,), jnp.float32)
    w_in, x_in, dy_in, row_in, col_in = draw_matrix(sub_keys[1], D_MODEL, D_FF)
    w_out, x_out, dy_out, row_out, col_out = draw_matrix(sub_keys[2], D_FF, D_MODEL)
    return {'hyper_params': hyper_params, 'w_in': w_in, 'x_in': x_in, 'dy_in': dy_in, 'row_in': row_in, 'col_in': col_in, 'w_out': w_out, 'x_out': x_out, 'dy_out': dy_out, 'row_out': row_out, 'col_out': col_out}


def adafactor_one(w_mat, x_act, dy_act, row_old, col_old, hyper_params):
    beta_two = hyper_params[0]
    rho_step = hyper_params[1]
    clip_max = hyper_params[2]
    grad_mat = jnp.dot(x_act.T, dy_act, preferred_element_type=jnp.float32)
    sq_grad = grad_mat * grad_mat + EPS_ONE
    row_new = beta_two * row_old + (1.0 - beta_two) * jnp.mean(sq_grad, axis=1)
    col_new = beta_two * col_old + (1.0 - beta_two) * jnp.mean(sq_grad, axis=0)
    row_mean = jnp.mean(row_new)
    update = grad_mat * lax.rsqrt((row_new / row_mean)[:, None] * col_new[None, :])
    upd_rms = jnp.sqrt(jnp.mean(update * update))
    w_rms = jnp.sqrt(jnp.mean(w_mat * w_mat))
    step_size = rho_step * jnp.maximum(EPS_TWO, w_rms) / jnp.maximum(1.0, upd_rms / clip_max)
    return w_mat - step_size * update, row_new, col_new


def reference(hyper_params, w_in, x_in, dy_in, row_in, col_in, w_out, x_out, dy_out, row_out, col_out):
    def one_layer(layer_args):
        w_first, x_first, dy_first, row_first, col_first, w_second, x_second, dy_second, row_second, col_second = layer_args
        in_result = adafactor_one(w_first, x_first, dy_first, row_first, col_first, hyper_params)
        out_result = adafactor_one(w_second, x_second, dy_second, row_second, col_second, hyper_params)
        return in_result + out_result
    results = lax.map(one_layer, (w_in, x_in, dy_in, row_in, col_in, w_out, x_out, dy_out, row_out, col_out))
    return (results[0], results[1], results[2], results[3], results[4], results[5])
```

```python
import functools

import jax
import jax.numpy as jnp
from jax import lax
from jax.experimental import pallas as pl
from jax.experimental.pallas import tpu as pltpu
from jax.sharding import PartitionSpec as P

EPS_ONE = 1e-30
EPS_TWO = 1e-3
MESH = pl.DeviceIdType.MESH
F32 = jnp.float32

SHARE = ((0, 1, 3, 4, 12, 16, 48, 5), (0, 1, 3, 4, 12, 16, 48, 60))
CODE = (0, 14, 33, 55, 24, 22, 57, 47)
PARTNERS = tuple(sorted({m for lst in SHARE for m in lst[1:]} | set(CODE[1:])))
N_BLOCK = 8
CHUNK = 1024
SCALE = 2.0 ** -20


def digit_xor(v, m):
    if m == 0:
        return v
    if m == 1:
        return v + 1 - 2 * (v % 2)
    if m == 2:
        return (v + 2) % 4
    return 3 - v


def fold(x):
    acc = x[:, 0:128]
    for i in range(1, x.shape[1] // 128):
        acc = acc + x[:, i * 128:(i + 1) * 128]
    return acc


def stats_kernel(dims, hyper, a0, a1, so0, so1, bo0, bo1, b0, b1, w0, w1,
                 g0, g1, c0, c1, r_out, s_out,
                 a_all, b_buf, gs, w_buf, so_buf, bo_buf, ar_buf, cnew, rs_own, rs_in, rs_core, rp_all,
                 sc_buf, sh_buf, k_buf,
                 b_sem, w_sem, in_sem, own_sem,
                 a_ss, a_rs, g_ss, g_rs, rs_ss, rs_rs, rp_ss, rp_rs, c_ss, c_rs,
                 ar_ss, ar_rs, sc_ss, sc_rs, sh_ss, sh_rs, k_ss, k_rs):
    tile, width, block, n_small, n_big = dims
    n_chunk = block // CHUNK
    col = lax.axis_index('col')
    row = lax.axis_index('row')
    x, y, z = row % 4, (row // 4) % 4, row // 16
    bx, by, bz = x // 2, y // 2, z // 2
    ax, ay, az = (x + bx) % 2, (y + by) % 2, (z + bz) % 2
    syn = (ax + by + az) % 2 + 2 * ((bx + ay + by) % 2) + 4 * ((ay + az + bz) % 2)
    rank = bx + 2 * bz + 4 * ay
    base = pl.multiple_of(syn * block, block)

    def peer(mask):
        return (col, digit_xor(z, mask // 16) * 16 + digit_xor(y, (mask // 4) % 4) * 4 + digit_xor(x, mask % 4))

    core = (1 - col, row)
    a_in, so_in, bo_in, b_in, w_in = (a0, a1), (so0, so1), (bo0, bo1), (b0, b1), (w0, w1)
    g_out, c_out = (g0, g1), (c0, c1)

    def rcopy(src, dst, ss, rs, dev):
        return pltpu.make_async_remote_copy(src_ref=src, dst_ref=dst, send_sem=ss, recv_sem=rs, device_id=dev, device_id_type=MESH)

    barrier = pltpu.get_barrier_semaphore()
    for mask in PARTNERS:
        pl.semaphore_signal(barrier, inc=1, device_id=peer(mask), device_id_type=MESH)
    pl.semaphore_signal(barrier, inc=1, device_id=core, device_id_type=MESH)

    a_load = [pltpu.make_async_copy(a_in[m], a_all.at[m, 0:tile], in_sem.at[m]) for m in range(2)]
    for cp in a_load:
        cp.start()

    def b_load(m, c):
        return pltpu.make_async_copy(b_in[m].at[:, pl.ds(pl.multiple_of(base + c * CHUNK, CHUNK), CHUNK)], b_buf.at[m, c], b_sem.at[m, c])

    for c in range(n_chunk):
        for m in range(2):
            b_load(m, c).start()
    misc = []
    for m in range(2):
        misc.append(pltpu.make_async_copy(so_in[m], so_buf.at[m], in_sem.at[2 + m]))
        misc.append(pltpu.make_async_copy(bo_in[m], bo_buf.at[m], in_sem.at[4 + m]))
        misc.append(pltpu.make_async_copy(w_in[m], w_buf.at[m], w_sem.at[m]))
    for cp in misc:
        cp.start()

    for cp in a_load:
        cp.wait()
    pl.semaphore_wait(barrier, len(PARTNERS) + 1)

    def a_copy(m, j):
        return rcopy(a_all.at[m, 0:tile], a_all.at[m, j * tile:(j + 1) * tile], a_ss.at[m, j], a_rs.at[m, j], peer(SHARE[m][j]))

    for m in range(2):
        for j in range(1, N_BLOCK):
            a_copy(m, j).start()

    def g_copy(m, j, lo, size):
        return rcopy(gs.at[m, j * tile:(j + 1) * tile, lo:lo + size], g_out[m].at[:, pl.ds(pl.multiple_of(base + lo, CHUNK), size)],
                     g_ss.at[m, j], g_rs.at[m, j], peer(SHARE[m][j]))

    def g_own(m, lo, size):
        return pltpu.make_async_copy(gs.at[m, 0:tile, lo:lo + size], g_out[m].at[:, pl.ds(pl.multiple_of(base + lo, CHUNK), size)], own_sem.at[m])

    def send_g(m, c):
        for j in range(1, N_BLOCK):
            g_copy(m, j, c * CHUNK, CHUNK).start()

    def compute(m, c):
        b_load(m, c).wait()
        g = jnp.dot(a_all[m], b_buf[m, c], preferred_element_type=F32)
        gs[m, :, c * CHUNK:(c + 1) * CHUNK] = g
        sq = g * g
        ar_buf[rank, :, m * block + c * CHUNK:m * block + (c + 1) * CHUNK] = jnp.sum(sq, axis=0, keepdims=True)
        part = fold(sq)
        if c == 0:
            rs_own[m] = part
        else:
            rs_own[m] = rs_own[m] + part

    for m in range(2):
        for j in range(1, N_BLOCK):
            a_copy(m, j).wait_recv()
    for c in range(n_chunk):
        for m in range(2):
            compute(m, c)
        if c == 0:
            send_g(0, 0)

    def rs_copy(m, j):
        return rcopy(rs_own.at[m, j * tile:(j + 1) * tile], rs_in.at[m, j * tile:(j + 1) * tile], rs_ss.at[m, j], rs_rs.at[m, j], peer(SHARE[m][j]))

    def ar_copy(j):
        return rcopy(ar_buf.at[rank], ar_buf.at[rank], ar_ss.at[j], ar_rs.at[j], peer(CODE[j]))

    for m in range(2):
        for j in range(1, N_BLOCK):
            rs_copy(m, j).start()
    for j in range(1, N_BLOCK):
        ar_copy(j).start()
    for m in range(2):
        g_own(m, 0, block).start()
    send_g(1, 0)

    w_load = [misc[2], misc[5]]
    for m in range(2):
        w_load[m].wait()

        def w_step(i, acc):
            blk = w_buf[m, :, pl.ds(pl.multiple_of(i * 1024, 1024), 1024)]
            return acc + fold(blk * blk)

        w_acc = lax.fori_loop(0, width // 1024, w_step, jnp.zeros((tile, 128), F32))
        sc_buf[0, 4 * m + 2:4 * m + 3, :] = jnp.sum(w_acc, axis=0, keepdims=True)
    for i in (0, 1, 3, 4):
        misc[i].wait()
    old0 = jnp.sum(so_buf[0], axis=1, keepdims=True) * (0.5 / 128)
    old1 = jnp.sum(bo_buf[1], axis=1, keepdims=True) * (1.0 / (64 * 128))
    sc_buf[0, 3:4, :] = jnp.broadcast_to(old0, (1, 128))
    sc_buf[0, 7:8, :] = jnp.broadcast_to(old1, (1, 128))
    for m in range(2):
        sc_buf[0, 4 * m + 1:4 * m + 2, :] = jnp.sum(rs_own[m], axis=0, keepdims=True)

    for m in range(2):
        for j in range(1, N_BLOCK):
            rs_copy(m, j).wait_recv()
        total = rs_own[m, 0:tile]
        for j in range(1, N_BLOCK):
            total = total + rs_in[m, j * tile:(j + 1) * tile]
        rs_core[0, m] = total
    core_rows = rcopy(rs_core.at[0], rs_core.at[1], k_ss.at[0], k_rs.at[0], core)
    core_rows.start()
    send_g(0, 1)
    core_rows.wait_recv()
    beta_two = hyper[0]
    rho_step = hyper[1]
    clip_max = hyper[2]
    eye = lax.broadcasted_iota(jnp.int32, (tile, tile), 0) == lax.broadcasted_iota(jnp.int32, (tile, tile), 1)
    for m in range(2):
        total = jnp.sum(rs_core[0, m] + rs_core[1, m], axis=1, keepdims=True)
        old = jnp.sum(jnp.where(eye, jnp.broadcast_to(so_buf[m], (tile, tile)), 0.0), axis=1, keepdims=True)
        new = beta_two * old + (1.0 - beta_two) * (total * (1.0 / n_big) + EPS_ONE)
        rp_all[m, 0:tile] = jnp.broadcast_to(new, (tile, 128))
        r_out[m] = jnp.broadcast_to(new, (tile, 128))

    def rp_copy(m, j):
        return rcopy(rp_all.at[m, 0:tile], rp_all.at[m, j * tile:(j + 1) * tile], rp_ss.at[m, j], rp_rs.at[m, j], peer(SHARE[m][j]))

    for m in range(2):
        for j in range(1, N_BLOCK):
            rp_copy(m, j).start()

    for j in range(1, N_BLOCK):
        ar_copy(j).wait()
    for m in range(2):
        lanes = slice(m * block, (m + 1) * block)
        total = ar_buf[0, :, lanes]
        for j in range(1, N_BLOCK):
            total = total + ar_buf[j, :, lanes]
        old = bo_buf[m, :, pl.ds(base, block)]
        cnew[m] = beta_two * old + (1.0 - beta_two) * (total * (1.0 / n_small) + EPS_ONE)

    def c_copy(m, j):
        return rcopy(cnew.at[m], c_out[m].at[:, pl.ds(base, block)], c_ss.at[m, j], c_rs.at[m, j], peer(SHARE[m][j]))

    c_own = [pltpu.make_async_copy(cnew.at[m], c_out[m].at[:, pl.ds(base, block)], in_sem.at[6 + m]) for m in range(2)]
    for m in range(2):
        for j in range(1, N_BLOCK):
            c_copy(m, j).start()
        c_own[m].start()

    for m in range(2):
        def u_step(i, acc):
            lanes = pl.ds(pl.multiple_of(i * 512, 512), 512)
            blk = gs[m, :, lanes]
            return acc + fold(blk * blk * (1.0 / cnew[m, :, lanes]))

        u_acc = lax.fori_loop(0, block // 512, u_step, jnp.zeros((N_BLOCK * tile, 128), F32))
        for j in range(1, N_BLOCK):
            rp_copy(m, j).wait()
        sc_buf[0, 4 * m:4 * m + 1, :] = jnp.sum(u_acc * SCALE / rp_all[m], axis=0, keepdims=True)

    def sc_copy(j):
        return rcopy(sc_buf.at[0], sc_buf.at[j], sc_ss.at[j], sc_rs.at[j], peer(CODE[j]))

    def sh_copy(j):
        return rcopy(sh_buf.at[0], sh_buf.at[j], sh_ss.at[j], sh_rs.at[j], peer(SHARE[0][j]))

    for j in range(1, N_BLOCK):
        sc_copy(j).start()
    send_g(1, 1)
    send_g(0, 2)
    for j in range(1, N_BLOCK):
        sc_copy(j).wait()
    total = sc_buf[0]
    for j in range(1, N_BLOCK):
        total = total + sc_buf[j]
    sh_buf[0] = total
    for j in range(1, N_BLOCK):
        sh_copy(j).start()
    send_g(1, 2)
    send_g(0, 3)
    send_g(1, 3)
    for j in range(1, N_BLOCK):
        sh_copy(j).wait()
    total = sh_buf[0]
    for j in range(1, N_BLOCK):
        total = total + sh_buf[j]
    k_buf[0] = total
    core_sum = rcopy(k_buf.at[0], k_buf.at[1], k_ss.at[1], k_rs.at[1], core)
    core_sum.start()
    core_sum.wait()
    sums = jnp.broadcast_to(jnp.sum(k_buf[0] + k_buf[1], axis=1, keepdims=True), (8, 128))
    n_total = float(n_small) * float(n_big)
    for m, n_rows in ((0, n_small), (1, n_big)):
        u_sum, g_sum, w_sum, r_sum = (sums[4 * m + i:4 * m + i + 1] for i in range(4))
        row_mean = beta_two * (r_sum * (1.0 / n_rows)) + (1.0 - beta_two) * (g_sum * (1.0 / n_total) + EPS_ONE)
        upd_rms = jnp.sqrt(u_sum * row_mean * (1.0 / (n_total * SCALE)))
        w_rms = jnp.sqrt(w_sum * (1.0 / n_total))
        step_size = rho_step * jnp.maximum(EPS_TWO, w_rms) / jnp.maximum(1.0, upd_rms / clip_max)
        s_out[m:m + 1, :] = step_size * jnp.sqrt(row_mean)

    core_rows.wait_send()
    for m in range(2):
        g_own(m, 0, block).wait()
        c_own[m].wait()
        for j in range(1, N_BLOCK):
            a_copy(m, j).wait_send()
            rs_copy(m, j).wait_send()
            c_copy(m, j).wait()
            g_copy(m, j, 0, block).wait()


def apply_kernel(g0, g1, w0, w1, c0, c1, r_new, scal, w0_new, w1_new, c0_new, c1_new, r0_new, r1_new):
    tile = w0.shape[0]
    for m, (g, w, c, w_new, c_new) in enumerate(((g0, w0, c0, w0_new, c0_new), (g1, w1, c1, w1_new, c1_new))):
        row_scale = scal[m:m + 1, 0:1] * lax.rsqrt(r_new[m, :, 0:1])
        w_new[...] = w[...] - (g[...] * lax.rsqrt(c[...])) * row_scale
        c_new[...] = c[...]

    @pl.when(pl.program_id(0) == 0)
    def _():
        eye = lax.broadcasted_iota(jnp.int32, (tile, tile), 0) == lax.broadcasted_iota(jnp.int32, (tile, tile), 1)
        for m, r_row in ((0, r0_new), (1, r1_new)):
            r_row[...] = jnp.sum(jnp.where(eye, r_new[m, :, 0:tile], 0.0), axis=0, keepdims=True)


def solution(mesh):
    tile_in = P(None, 'row', 'col')
    tile_out = P(None, 'col', 'row')
    lane_row = P(None, None, 'row')
    lane_col = P(None, None, 'col')
    vec_row = P(None, 'row')
    vec_col = P(None, 'col')
    n_row = mesh.shape['row']
    n_col = mesh.shape['col']

    def local_step(hyper_params, w_in, x_in, dy_in, row_in, col_in, w_out, x_out, dy_out, row_out, col_out):
        tile, width = w_in.shape[1], w_in.shape[2]
        tokens = x_in.shape[1]
        block = width // N_BLOCK
        n_chunk = block // CHUNK
        dims = (tile, width, block, tile * n_row, width * n_col)
        rows = N_BLOCK * tile
        w0 = w_in[0]
        w1 = jnp.transpose(w_out[0])
        a0 = jnp.transpose(x_in[0])
        a1 = jnp.transpose(dy_out[0])
        dma = pltpu.SemaphoreType.DMA
        any_spec = pl.BlockSpec(memory_space=pl.ANY)
        hbm_spec = pl.BlockSpec(memory_space=pltpu.HBM)
        vmem_spec = pl.BlockSpec(memory_space=pltpu.VMEM)
        g0, g1, c0, c1, r_new, scal = pl.pallas_call(
            functools.partial(stats_kernel, dims),
            out_shape=(
                jax.ShapeDtypeStruct((tile, width), F32),
                jax.ShapeDtypeStruct((tile, width), F32),
                jax.ShapeDtypeStruct((1, width), F32),
                jax.ShapeDtypeStruct((1, width), F32),
                jax.ShapeDtypeStruct((2, tile, 128), F32),
                jax.ShapeDtypeStruct((8, 128), F32),
            ),
            in_specs=[pl.BlockSpec(memory_space=pltpu.SMEM)] + [any_spec] * 10,
            out_specs=(hbm_spec, hbm_spec, hbm_spec, hbm_spec, vmem_spec, vmem_spec),
            scratch_shapes=[
                pltpu.VMEM((2, rows, tokens), jnp.bfloat16),
                pltpu.VMEM((2, n_chunk, tokens, CHUNK), jnp.bfloat16),
                pltpu.VMEM((2, rows, block), F32),
                pltpu.VMEM((2, tile, width), F32),
                pltpu.VMEM((2, 1, tile), F32),
                pltpu.VMEM((2, 1, width), F32),
                pltpu.VMEM((N_BLOCK, 1, 2 * block), F32),
                pltpu.VMEM((2, 1, block), F32),
                pltpu.VMEM((2, rows, 128), F32),
                pltpu.VMEM((2, rows, 128), F32),
                pltpu.VMEM((2, 2, tile, 128), F32),
                pltpu.VMEM((2, rows, 128), F32),
                pltpu.VMEM((N_BLOCK, 8, 128), F32),
                pltpu.VMEM((N_BLOCK, 8, 128), F32),
                pltpu.VMEM((2, 8, 128), F32),
                dma((2, n_chunk)), dma((2,)), dma((8,)), dma((2,)),
                dma((2, 8)), dma((2, 8)), dma((2, 8)), dma((2, 8)), dma((2, 8)), dma((2, 8)),
                dma((2, 8)), dma((2, 8)), dma((2, 8)), dma((2, 8)),
                dma((8,)), dma((8,)), dma((8,)), dma((8,)), dma((8,)), dma((8,)), dma((2,)), dma((2,)),
            ],
            compiler_params=pltpu.CompilerParams(collective_id=0, has_side_effects=True, vmem_limit_bytes=48 * 1024 * 1024),
            name='stats',
        )(hyper_params, a0, a1, row_in, col_out, col_in, row_out, dy_in[0], x_out[0], w0, w1)

        step = 4096
        tile_spec = pl.BlockSpec((tile, step), lambda i: (0, i))
        vec_spec = pl.BlockSpec((1, step), lambda i: (0, i))
        w0_new, w1_new, c0_new, c1_new, r0_new, r1_new = pl.pallas_call(
            apply_kernel,
            grid=(width // step,),
            out_shape=(
                jax.ShapeDtypeStruct((tile, width), F32),
                jax.ShapeDtypeStruct((tile, width), F32),
                jax.ShapeDtypeStruct((1, width), F32),
                jax.ShapeDtypeStruct((1, width), F32),
                jax.ShapeDtypeStruct((1, tile), F32),
                jax.ShapeDtypeStruct((1, tile), F32),
            ),
            in_specs=[tile_spec, tile_spec, tile_spec, tile_spec, vec_spec, vec_spec,
                      pl.BlockSpec((2, tile, 128), lambda i: (0, 0, 0)), pl.BlockSpec((8, 128), lambda i: (0, 0))],
            out_specs=(tile_spec, tile_spec, vec_spec, vec_spec,
                       pl.BlockSpec((1, tile), lambda i: (0, 0)), pl.BlockSpec((1, tile), lambda i: (0, 0))),
            name='apply',
        )(g0, g1, w0, w1, c0, c1, r_new, scal)
        return w0_new[None], r0_new, c0_new, jnp.transpose(w1_new)[None], c1_new, r1_new

    return jax.shard_map(local_step, mesh=mesh, in_specs=(P(), tile_in, lane_row, lane_col, vec_row, vec_col, tile_out, lane_col, lane_row, vec_col, vec_row), out_specs=(tile_in, vec_row, vec_col, tile_out, vec_col, vec_row), check_vma=False)
```

```python
import functools

import jax
import jax.numpy as jnp
from jax import lax
from jax.experimental import pallas as pl
from jax.experimental.pallas import tpu as pltpu
from jax.sharding import PartitionSpec as P

EPS_ONE = 1e-30
EPS_TWO = 1e-3
MESH = pl.DeviceIdType.MESH
F32 = jnp.float32

SHARE = ((0, 1, 3, 4, 12, 16, 48, 5), (0, 1, 3, 4, 12, 16, 48, 60))
CODE = (0, 14, 33, 55, 24, 22, 57, 47)
PARTNERS = tuple(sorted({m for lst in SHARE for m in lst[1:]} | set(CODE[1:])))
FAR_PARTNERS = tuple(sorted({m for lst in SHARE for m in lst}))
N_BLOCK = 8
CHUNK = 1024
SCALE = 2.0 ** -20


def digit_xor(v, m):
    if m == 0:
        return v
    if m == 1:
        return v + 1 - 2 * (v % 2)
    if m == 2:
        return (v + 2) % 4
    return 3 - v


def fold(x):
    acc = x[:, 0:128]
    for i in range(1, x.shape[1] // 128):
        acc = acc + x[:, i * 128:(i + 1) * 128]
    return acc


def stats_kernel(dims, hyper, a0, a1, so0, so1, bo0, bo1, b0, b1, w0, w1,
                 g0, g1, c0, c1, wv0, wv1, r_out, s_out,
                 a_all, b_buf, b_far, gs, so_buf, bo_buf, ar_buf, cnew, rs_own, rs_in, rs_far, rp_all,
                 sc_buf, sh_buf, sf_buf,
                 b_sem, w_sem, in_sem, own_sem,
                 a_ss, a_rs, g_ss, g_rs, rs_ss, rs_rs, rf_ss, rf_rs, rp_ss, rp_rs, c_ss, c_rs,
                 ar_ss, ar_rs, sc_ss, sc_rs, sh_ss, sh_rs, sf_ss, sf_rs):
    tile, width, block, n_small, n_big = dims
    n_chunk = block // CHUNK
    col = lax.axis_index('col')
    row = lax.axis_index('row')
    x, y, z = row % 4, (row // 4) % 4, row // 16
    bx, by, bz = x // 2, y // 2, z // 2
    ax, ay, az = (x + bx) % 2, (y + by) % 2, (z + bz) % 2
    syn = (ax + by + az) % 2 + 2 * ((bx + ay + by) % 2) + 4 * ((ay + az + bz) % 2)
    rank = bx + 2 * bz + 4 * ay
    base = pl.multiple_of(syn * block, block)
    base_far = pl.multiple_of((N_BLOCK - 1 - syn) * block, block)
    peers = range(1, N_BLOCK)
    links = range(1, N_BLOCK - 1)

    def peer_row(mask):
        return digit_xor(z, mask // 16) * 16 + digit_xor(y, (mask // 4) % 4) * 4 + digit_xor(x, mask % 4)

    def near(mask):
        return (col, peer_row(mask))

    def far(mask):
        return (1 - col, peer_row(mask))

    a_in, so_in, bo_in, b_in, w_in = (a0, a1), (so0, so1), (bo0, bo1), (b0, b1), (w0, w1)
    g_out, c_out, wv = (g0, g1), (c0, c1), (wv0, wv1)

    def rcopy(src, dst, ss, rs, dev):
        return pltpu.make_async_remote_copy(src_ref=src, dst_ref=dst, send_sem=ss, recv_sem=rs, device_id=dev, device_id_type=MESH)

    barrier = pltpu.get_barrier_semaphore()
    for mask in PARTNERS:
        pl.semaphore_signal(barrier, inc=1, device_id=near(mask), device_id_type=MESH)
    for mask in FAR_PARTNERS:
        pl.semaphore_signal(barrier, inc=1, device_id=far(mask), device_id_type=MESH)

    a_load = [pltpu.make_async_copy(a_in[m], a_all.at[m, 0:tile], in_sem.at[m]) for m in range(2)]
    for cp in a_load:
        cp.start()

    def b_load(m, c):
        return pltpu.make_async_copy(b_in[m].at[:, pl.ds(pl.multiple_of(base + c * CHUNK, CHUNK), CHUNK)],
                                     b_buf.at[m, :, c * CHUNK:(c + 1) * CHUNK], b_sem.at[m, c])

    def b_far_load(m):
        return pltpu.make_async_copy(b_in[m].at[:, pl.ds(base_far, block)], b_far.at[m], b_sem.at[m, n_chunk])

    so_load = [pltpu.make_async_copy(so_in[m], so_buf.at[m], in_sem.at[2 + m]) for m in range(2)]
    bo_load = [pltpu.make_async_copy(bo_in[m], bo_buf.at[m], in_sem.at[4 + m]) for m in range(2)]
    w_load = [pltpu.make_async_copy(w_in[m], wv[m], w_sem.at[m]) for m in range(2)]
    for cp in a_load:
        cp.wait()
    for c in range(n_chunk):
        b_load(0, c).start()
    with jax.named_scope('p00_barrier'):
        pl.semaphore_wait(barrier, len(PARTNERS) + len(FAR_PARTNERS))

    def rows_of(j):
        return slice(j * tile, (j + 1) * tile)

    def a_copy(m, j):
        return rcopy(a_all.at[m, 0:tile], a_all.at[m, rows_of(j)], a_ss.at[m, j], a_rs.at[m, j], near(SHARE[m][j]))

    for m in range(2):
        for j in peers:
            a_copy(m, j).start()
    for c in range(n_chunk):
        b_load(1, c).start()
    for cp in so_load + bo_load + w_load:
        cp.start()
    for m in range(2):
        b_far_load(m).start()

    def g_copy(m, j, lo, size):
        return rcopy(gs.at[m, rows_of(j), lo:lo + size], g_out[m].at[:, pl.ds(pl.multiple_of(base + lo, CHUNK), size)],
                     g_ss.at[m, j], g_rs.at[m, j], near(SHARE[m][j]))

    def send_g(*portions):
        for m, c in portions:
            for j in links:
                g_copy(m, j, c * CHUNK, CHUNK).start()

    def rs_copy(m, j):
        return rcopy(rs_own.at[m, rows_of(j)], rs_in.at[m, rows_of(j)], rs_ss.at[m, j], rs_rs.at[m, j], near(SHARE[m][j]))

    def rf_copy(m, j):
        return rcopy(rs_own.at[m, rows_of(j)], rs_far.at[m, rows_of(j)], rf_ss.at[m, j], rf_rs.at[m, j], far(SHARE[m][j]))

    def ar_copy(m, j):
        return rcopy(ar_buf.at[m, rank], ar_buf.at[m, rank], ar_ss.at[m, j], ar_rs.at[m, j], near(CODE[j]))

    def rp_copy(m, j):
        return rcopy(rp_all.at[m, 0:tile], rp_all.at[m, rows_of(j)], rp_ss.at[m, j], rp_rs.at[m, j], near(SHARE[m][j]))

    def c_copy(m, j):
        return rcopy(cnew.at[m], c_out[m].at[:, pl.ds(base, block)], c_ss.at[m, j], c_rs.at[m, j], near(SHARE[m][j]))

    def sc_copy(j):
        return rcopy(sc_buf.at[0], sc_buf.at[j], sc_ss.at[j], sc_rs.at[j], near(CODE[j]))

    def sh_copy(j):
        return rcopy(sh_buf.at[0], sh_buf.at[j], sh_ss.at[j], sh_rs.at[j], near(SHARE[0][j]))

    def sf_copy(j):
        return rcopy(sh_buf.at[0], sf_buf.at[j], sf_ss.at[j], sf_rs.at[j], far(SHARE[0][j]))

    def products(m):
        for h in range(n_chunk // 2):
            for c in (2 * h, 2 * h + 1):
                b_load(m, c).wait()
            lanes = slice(2 * h * CHUNK, 2 * (h + 1) * CHUNK)
            g = jnp.dot(a_all[m], b_buf[m, :, lanes], preferred_element_type=F32)
            gs[m, :, lanes] = g
            sq = g * g
            ar_buf[m, rank, :, lanes] = jnp.sum(sq, axis=0, keepdims=True)
            part = fold(sq)
            rs_own[m] = part if h == 0 else rs_own[m] + part

    def products_far(m):
        b_far_load(m).wait()
        g_out[m][:, pl.ds(base_far, block)] = jnp.dot(a_all[m, 0:tile], b_far[m], preferred_element_type=F32)

    def send_sums(m):
        for j in peers:
            rs_copy(m, j).start()
        for j in range(N_BLOCK):
            rf_copy(m, j).start()
        for j in peers:
            ar_copy(m, j).start()

    with jax.named_scope('p01_a_wait0'):
        for j in peers:
            a_copy(0, j).wait_recv()
    with jax.named_scope('p02_products0'):
        products(0)
    send_sums(0)
    with jax.named_scope('p03_a_wait1'):
        for j in peers:
            a_copy(1, j).wait_recv()
    with jax.named_scope('p04_products1'):
        products(1)
    send_sums(1)
    send_g((0, 0))
    for m in range(2):
        g_out[m][:, pl.ds(base, block)] = gs[m, 0:tile]

    with jax.named_scope('p04_wsum'):
        for m in range(2):
            w_load[m].wait()

            def w_step(i, acc):
                blk = wv[m][:, pl.ds(pl.multiple_of(i * 1024, 1024), 1024)]
                return acc + fold(blk * blk)

            w_acc = lax.fori_loop(0, width // 1024, w_step, jnp.zeros((tile, 128), F32))
            sc_buf[0, 4 * m + 2:4 * m + 3, :] = jnp.sum(w_acc, axis=0, keepdims=True)
            bo_load[m].wait()
            so_load[m].wait()
        old0 = jnp.sum(so_buf[0], axis=1, keepdims=True) * (0.5 / 128)
        old1 = jnp.sum(bo_buf[1], axis=1, keepdims=True) * (1.0 / (64 * 128))
        sc_buf[0, 3:4, :] = jnp.broadcast_to(old0, (1, 128))
        sc_buf[0, 7:8, :] = jnp.broadcast_to(old1, (1, 128))
        for m in range(2):
            sc_buf[0, 4 * m + 1:4 * m + 2, :] = jnp.sum(rs_own[m], axis=0, keepdims=True)

    beta_two = hyper[0]
    rho_step = hyper[1]
    clip_max = hyper[2]
    eye = lax.broadcasted_iota(jnp.int32, (tile, tile), 0) == lax.broadcasted_iota(jnp.int32, (tile, tile), 1)
    for m in range(2):
        with jax.named_scope('p05_rs_wait%d' % m):
            for j in peers:
                rs_copy(m, j).wait_recv()
            for j in range(N_BLOCK):
                rf_copy(m, j).wait_recv()
        total = rs_own[m, 0:tile]
        for j in peers:
            total = total + rs_in[m, rows_of(j)]
        total_far = rs_far[m, 0:tile]
        for j in peers:
            total_far = total_far + rs_far[m, rows_of(j)]
        total = jnp.sum(total + total_far, axis=1, keepdims=True)
        old = jnp.sum(jnp.where(eye, jnp.broadcast_to(so_buf[m], (tile, tile)), 0.0), axis=1, keepdims=True)
        new = beta_two * old + (1.0 - beta_two) * (total * (1.0 / n_big) + EPS_ONE)
        rp_all[m, 0:tile] = jnp.broadcast_to(new, (tile, 128))
        r_out[m] = jnp.broadcast_to(new, (tile, 128))
        for j in peers:
            rp_copy(m, j).start()
    send_g((0, 1), (0, 2))

    with jax.named_scope('p06_far0'):
        products_far(0)
    for m in range(2):
        if m == 1:
            with jax.named_scope('p06_far1'):
                products_far(1)
        with jax.named_scope('p07_ar_wait%d' % m):
            for j in peers:
                ar_copy(m, j).wait()
        with jax.named_scope('p08_cnew%d' % m):
            total = ar_buf[m, 0]
            for j in peers:
                total = total + ar_buf[m, j]
            old = bo_buf[m, :, pl.ds(base, block)]
            new = beta_two * old + (1.0 - beta_two) * (total * (1.0 / n_small) + EPS_ONE)
            cnew[m] = new
            c_out[m][:, pl.ds(base, block)] = new
        for j in peers:
            c_copy(m, j).start()
        with jax.named_scope('p09_u%d' % m):
            def u_step(i, acc):
                lanes = pl.ds(pl.multiple_of(i * 512, 512), 512)
                blk = gs[m, :, lanes]
                return acc + fold(blk * blk * (1.0 / cnew[m, :, lanes]))

            u_acc = lax.fori_loop(0, block // 512, u_step, jnp.zeros((N_BLOCK * tile, 128), F32))
        with jax.named_scope('p10_rp%d' % m):
            for j in peers:
                rp_copy(m, j).wait()
        sc_buf[0, 4 * m:4 * m + 1, :] = jnp.sum(u_acc * SCALE / rp_all[m], axis=0, keepdims=True)

    for j in peers:
        sc_copy(j).start()
    send_g((0, 3), (1, 0), (1, 1))
    with jax.named_scope('p11_sc_wait'):
        for j in peers:
            sc_copy(j).wait()
    total = sc_buf[0]
    for j in peers:
        total = total + sc_buf[j]
    sh_buf[0] = total
    for j in peers:
        sh_copy(j).start()
    for j in range(N_BLOCK):
        sf_copy(j).start()
    send_g((1, 2), (1, 3))
    with jax.named_scope('p12_sh_wait'):
        for j in peers:
            sh_copy(j).wait()
        for j in range(N_BLOCK):
            sf_copy(j).wait()
    total = sh_buf[0] + sf_buf[0]
    for j in peers:
        total = total + (sh_buf[j] + sf_buf[j])
    sums = jnp.broadcast_to(jnp.sum(total, axis=1, keepdims=True), (8, 128))
    n_total = float(n_small) * float(n_big)
    for m, n_rows in ((0, n_small), (1, n_big)):
        u_sum, g_sum, w_sum, r_sum = (sums[4 * m + i:4 * m + i + 1] for i in range(4))
        row_mean = beta_two * (r_sum * (1.0 / n_rows)) + (1.0 - beta_two) * (g_sum * (1.0 / n_total) + EPS_ONE)
        upd_rms = jnp.sqrt(u_sum * row_mean * (1.0 / (n_total * SCALE)))
        w_rms = jnp.sqrt(w_sum * (1.0 / n_total))
        step_size = rho_step * jnp.maximum(EPS_TWO, w_rms) / jnp.maximum(1.0, upd_rms / clip_max)
        s_out[m:m + 1, :] = step_size * jnp.sqrt(row_mean)

    with jax.named_scope('p13_final'):
        for m in range(2):
            rf_copy(m, 0).wait_send()
            for j in peers:
                a_copy(m, j).wait_send()
                rs_copy(m, j).wait_send()
                rf_copy(m, j).wait_send()
                c_copy(m, j).wait()
            for j in links:
                g_copy(m, j, 0, block).wait()


def apply_kernel(g0, g1, w0, w1, c0, c1, r_new, scal, w0_new, w1_new, c0_new, c1_new, r0_new, r1_new,
                 w_buf, r_buf, w_sem, c_sem, r_sem):
    tile, width = w0.shape
    step = 4096
    eye = lax.broadcasted_iota(jnp.int32, (tile, tile), 0) == lax.broadcasted_iota(jnp.int32, (tile, tile), 1)
    c_new, r_out, w_new = (c0_new, c1_new), (r0_new, r1_new), (w0_new, w1_new)
    c_old = (c0, c1)
    copies = [pltpu.make_async_copy(c_old[m], c_new[m], c_sem.at[m]) for m in range(2)]
    for m in range(2):
        copies[m].start()
        r_buf[m] = jnp.sum(jnp.where(eye, r_new[m, :, 0:tile], 0.0), axis=0, keepdims=True)
    for m, (g, w, c) in enumerate(((g0, w0, c0), (g1, w1, c1))):
        row_scale = scal[m:m + 1, 0:1] * lax.rsqrt(r_new[m, :, 0:1])
        for i in range(width // step):
            lanes = slice(i * step, (i + 1) * step)
            w_buf[m, :, lanes] = w[:, lanes] - (g[:, lanes] * lax.rsqrt(c[:, lanes])) * row_scale
            copies.append(pltpu.make_async_copy(w_buf.at[m, :, lanes], w_new[m].at[:, lanes], w_sem.at[m, i]))
            copies[-1].start()
    for m in range(2):
        copies.append(pltpu.make_async_copy(r_buf.at[m], r_out[m], r_sem.at[m]))
        copies[-1].start()
    for cp in copies:
        cp.wait()


def solution(mesh):
    tile_in = P(None, 'row', 'col')
    tile_out = P(None, 'col', 'row')
    lane_row = P(None, None, 'row')
    lane_col = P(None, None, 'col')
    vec_row = P(None, 'row')
    vec_col = P(None, 'col')
    n_row = mesh.shape['row']
    n_col = mesh.shape['col']

    def local_step(hyper_params, w_in, x_in, dy_in, row_in, col_in, w_out, x_out, dy_out, row_out, col_out):
        tile, width = w_in.shape[1], w_in.shape[2]
        tokens = x_in.shape[1]
        block = width // N_BLOCK
        n_chunk = block // CHUNK
        dims = (tile, width, block, tile * n_row, width * n_col)
        rows = N_BLOCK * tile
        w0 = w_in[0]
        w1 = jnp.transpose(w_out[0])
        a0 = jnp.transpose(x_in[0])
        a1 = jnp.transpose(dy_out[0])
        dma = pltpu.SemaphoreType.DMA
        any_spec = pl.BlockSpec(memory_space=pl.ANY)
        hbm_spec = pl.BlockSpec(memory_space=pltpu.HBM)
        vmem_spec = pl.BlockSpec(memory_space=pltpu.VMEM)
        big = jax.ShapeDtypeStruct((tile, width), F32)
        vec = jax.ShapeDtypeStruct((1, width), F32)
        short = jax.ShapeDtypeStruct((1, tile), F32)
        g0, g1, c0, c1, wv0, wv1, r_new, scal = pl.pallas_call(
            functools.partial(stats_kernel, dims),
            out_shape=(big, big, vec, vec, big, big, jax.ShapeDtypeStruct((2, tile, 128), F32), jax.ShapeDtypeStruct((8, 128), F32)),
            in_specs=[pl.BlockSpec(memory_space=pltpu.SMEM)] + [hbm_spec] * 10,
            out_specs=(vmem_spec,) * 8,
            scratch_shapes=[
                pltpu.VMEM((2, rows, tokens), jnp.bfloat16),
                pltpu.VMEM((2, tokens, block), jnp.bfloat16),
                pltpu.VMEM((2, tokens, block), jnp.bfloat16),
                pltpu.VMEM((2, rows, block), F32),
                pltpu.VMEM((2, 1, tile), F32),
                pltpu.VMEM((2, 1, width), F32),
                pltpu.VMEM((2, N_BLOCK, 1, block), F32),
                pltpu.VMEM((2, 1, block), F32),
                pltpu.VMEM((2, rows, 128), F32),
                pltpu.VMEM((2, rows, 128), F32),
                pltpu.VMEM((2, rows, 128), F32),
                pltpu.VMEM((2, rows, 128), F32),
                pltpu.VMEM((N_BLOCK, 8, 128), F32),
                pltpu.VMEM((N_BLOCK, 8, 128), F32),
                pltpu.VMEM((N_BLOCK, 8, 128), F32),
                dma((2, n_chunk + 1)), dma((2,)), dma((8,)), dma((2,)),
            ] + [dma((2, 8))] * 14 + [dma((8,))] * 6,
            compiler_params=pltpu.CompilerParams(collective_id=0, has_side_effects=True, vmem_limit_bytes=40 * 1024 * 1024),
            name='stats',
        )(*[pltpu.with_memory_space_constraint(v, pltpu.HBM) for v in (hyper_params, a0, a1, row_in, col_out, col_in, row_out, dy_in[0], x_out[0], w0, w1)])

        n_step = width // 4096
        w0_new, w1_new, c0_new, c1_new, r0_new, r1_new = pl.pallas_call(
            apply_kernel,
            out_shape=(big, big, vec, vec, short, short),
            in_specs=[vmem_spec] * 8,
            out_specs=(hbm_spec,) * 6,
            scratch_shapes=[pltpu.VMEM((2, tile, width), F32), pltpu.VMEM((2, 1, tile), F32), dma((2, n_step)), dma((2,)), dma((2,))],
            compiler_params=pltpu.CompilerParams(vmem_limit_bytes=6 * 1024 * 1024),
            name='apply',
        )(g0, g1, wv0, wv1, c0, c1, r_new, scal)
        return w0_new[None], r0_new, c0_new, jnp.transpose(w1_new)[None], c1_new, r1_new

    return jax.shard_map(local_step, mesh=mesh, in_specs=(P(), tile_in, lane_row, lane_col, vec_row, vec_col, tile_out, lane_col, lane_row, vec_col, vec_row), out_specs=(tile_in, vec_row, vec_col, tile_out, vec_col, vec_row), check_vma=False)
```

```python
import functools

import jax
import jax.numpy as jnp
from jax import lax
from jax.experimental import pallas as pl
from jax.experimental.pallas import tpu as pltpu
from jax.sharding import PartitionSpec as P

EPS_ONE = 1e-30
EPS_TWO = 1e-3
MESH = pl.DeviceIdType.MESH
F32 = jnp.float32

SHARE = ((0, 1, 3, 4, 12, 16, 48, 5), (0, 1, 3, 4, 12, 16, 48, 60))
CODE = (0, 14, 33, 55, 24, 22, 57, 47)
PARTNERS = tuple(sorted({m for lst in SHARE for m in lst[1:]} | set(CODE[1:])))
FAR_PARTNERS = tuple(sorted({m for lst in SHARE for m in lst}))
N_BLOCK = 8
CHUNK = 1024
SCALE = 2.0 ** -20


def digit_xor(v, m):
    if m == 0:
        return v
    if m == 1:
        return v + 1 - 2 * (v % 2)
    if m == 2:
        return (v + 2) % 4
    return 3 - v


def fold(x):
    acc = x[:, 0:128]
    for i in range(1, x.shape[1] // 128):
        acc = acc + x[:, i * 128:(i + 1) * 128]
    return acc


def stats_kernel(dims, hyper_in, a0, a1, so0, so1, bo0, bo1, b0, b1, w0, w1,
                 g0, g1, c0, c1, wv0, wv1, r_out, s_out,
                 hyper, a_all, b_buf, b_far, gs, so_buf, bo_buf, ar_buf, cnew, rs_own, rs_in, rp_all,
                 sc_buf, sh_buf,
                 sem_b, sem_w, sem_in, sem_pair, sem_one):
    tile, width, block, n_small, n_big = dims
    n_chunk = block // CHUNK
    col = lax.axis_index('col')
    row = lax.axis_index('row')
    x, y, z = row % 4, (row // 4) % 4, row // 16
    bx, by, bz = x // 2, y // 2, z // 2
    ax, ay, az = (x + bx) % 2, (y + by) % 2, (z + bz) % 2
    syn = (ax + by + az) % 2 + 2 * ((bx + ay + by) % 2) + 4 * ((ay + az + bz) % 2)
    rank = bx + 2 * bz + 4 * ay
    base = pl.multiple_of(syn * block, block)
    base_far = pl.multiple_of((N_BLOCK - 1 - syn) * block, block)
    peers = (N_BLOCK - 1,) + tuple(range(1, N_BLOCK - 1))
    a_rs, g_rs, rs_rs, rp_rs, c_rs, ar_rs = (lambda m, i=i: sem_pair.at[i, m] for i in range(6))
    a_ss, g_ss, rs_ss, rp_ss, c_ss, ar_ss, sc_ss, sh_ss, sc_rs, sh_rs = (sem_one.at[i] for i in range(10))
    links = range(1, N_BLOCK - 1)

    def peer_row(mask):
        return digit_xor(z, mask // 16) * 16 + digit_xor(y, (mask // 4) % 4) * 4 + digit_xor(x, mask % 4)

    def near(mask):
        return (col, peer_row(mask))

    def far(mask):
        return (1 - col, peer_row(mask))

    a_in, so_in, bo_in, b_in, w_in = (a0, a1), (so0, so1), (bo0, bo1), (b0, b1), (w0, w1)
    g_out, c_out, wv = (g0, g1), (c0, c1), (wv0, wv1)

    def rcopy(src, dst, ss, rs, dev):
        return pltpu.make_async_remote_copy(src_ref=src, dst_ref=dst, send_sem=ss, recv_sem=rs, device_id=dev, device_id_type=MESH)

    barrier = pltpu.get_barrier_semaphore()
    for mask in PARTNERS:
        pl.semaphore_signal(barrier, inc=1, device_id=near(mask), device_id_type=MESH)
    for mask in FAR_PARTNERS:
        pl.semaphore_signal(barrier, inc=1, device_id=far(mask), device_id_type=MESH)

    def drain(ref, sem):
        pltpu.make_async_copy(ref, ref, sem).wait()

    a_load = [pltpu.make_async_copy(a_in[m], a_all.at[m, 0:tile], sem_in.at[0]) for m in range(2)]
    for cp in a_load:
        cp.start()

    def b_load(m, c):
        return pltpu.make_async_copy(b_in[m].at[:, pl.ds(pl.multiple_of(base + c * CHUNK, CHUNK), CHUNK)],
                                     b_buf.at[m, :, c * CHUNK:(c + 1) * CHUNK], sem_b.at[m])

    def b_far_load(m):
        return pltpu.make_async_copy(b_in[m].at[:, pl.ds(base_far, block)], b_far.at[m], sem_b.at[2 + m])

    so_load = [pltpu.make_async_copy(so_in[m], so_buf.at[m], sem_in.at[1]) for m in range(2)]
    bo_load = [pltpu.make_async_copy(bo_in[m], bo_buf.at[m], sem_in.at[2]) for m in range(2)]
    w_load = [pltpu.make_async_copy(w_in[m], wv[m], sem_w.at[m]) for m in range(2)]
    hyper_load = pltpu.make_async_copy(hyper_in, hyper, sem_in.at[3])
    hyper_load.start()
    drain(a_all.at[:, 0:tile], sem_in.at[0])
    for c in range(n_chunk):
        b_load(0, c).start()
    with jax.named_scope('p00_barrier'):
        pl.semaphore_wait(barrier, len(PARTNERS) + len(FAR_PARTNERS))

    def rows_of(j):
        return slice(j * tile, (j + 1) * tile)

    def a_copy(m, j):
        return rcopy(a_all.at[m, 0:tile], a_all.at[m, rows_of(j)], a_ss, a_rs(m), near(SHARE[m][j]))

    for m in range(2):
        for j in peers:
            a_copy(m, j).start()
    for c in range(n_chunk):
        b_load(1, c).start()
    for cp in so_load + bo_load + w_load:
        cp.start()

    def g_copy(m, j, lo, size):
        return rcopy(gs.at[m, rows_of(j), lo:lo + size], g_out[m].at[:, pl.ds(pl.multiple_of(base + lo, CHUNK), size)],
                     g_ss, g_rs(m), near(SHARE[m][j]))

    def send_g(*portions):
        for m, c in portions:
            for j in links:
                g_copy(m, j, c * CHUNK, CHUNK).start()

    def rs_copy(m, j):
        return rcopy(rs_own.at[m, rows_of(j)], rs_in.at[m, rows_of(j)], rs_ss, rs_rs(m), near(SHARE[m][j]))

    def rf_copy(m, j):
        return rcopy(rs_own.at[m, rows_of(j)], rs_in.at[m, rows_of(N_BLOCK + j)], rs_ss, rs_rs(m), far(SHARE[m][j]))

    def ar_copy(m, j):
        return rcopy(ar_buf.at[m, rank], ar_buf.at[m, rank], ar_ss, ar_rs(m), near(CODE[j]))

    def rp_copy(m, j):
        return rcopy(rp_all.at[m, 0:tile], rp_all.at[m, rows_of(j)], rp_ss, rp_rs(m), near(SHARE[m][j]))

    def c_copy(m, j):
        return rcopy(cnew.at[m], c_out[m].at[:, pl.ds(base, block)], c_ss, c_rs(m), near(SHARE[m][j]))

    def sc_copy(j):
        return rcopy(sc_buf.at[0], sc_buf.at[j], sc_ss, sc_rs, near(CODE[j]))

    def sh_copy(j):
        return rcopy(sh_buf.at[0], sh_buf.at[j], sh_ss, sh_rs, near(SHARE[0][j]))

    def sf_copy(j):
        return rcopy(sh_buf.at[0], sh_buf.at[N_BLOCK + j], sh_ss, sh_rs, far(SHARE[0][j]))

    def products(m):
        drain(b_buf.at[m], sem_b.at[m])
        for h in range(n_chunk // 2):
            lanes = slice(2 * h * CHUNK, 2 * (h + 1) * CHUNK)
            g = jnp.dot(a_all[m], b_buf[m, :, lanes], preferred_element_type=F32)
            gs[m, :, lanes] = g
            sq = g * g
            ar_buf[m, rank, :, lanes] = jnp.sum(sq, axis=0, keepdims=True)
            part = fold(sq)
            rs_own[m] = part if h == 0 else rs_own[m] + part

    def products_far(m):
        b_far_load(m).wait()
        g_out[m][:, pl.ds(base_far, block)] = jnp.dot(a_all[m, 0:tile], b_far[m], preferred_element_type=F32)

    def send_sums(m):
        for j in peers:
            rs_copy(m, j).start()
        for j in peers + (0,):
            rf_copy(m, j).start()
        for j in peers:
            ar_copy(m, j).start()

    with jax.named_scope('p01_a_wait0'):
        drain(a_all.at[0, tile:N_BLOCK * tile], a_rs(0))
    with jax.named_scope('p02_products0'):
        products(0)
    send_sums(0)
    with jax.named_scope('p03_a_wait1'):
        drain(a_all.at[1, tile:N_BLOCK * tile], a_rs(1))
    with jax.named_scope('p04_products1'):
        products(1)
    send_sums(1)
    for m in range(2):
        b_far_load(m).start()
    for m in range(2):
        g_out[m][:, pl.ds(base, block)] = gs[m, 0:tile]

    with jax.named_scope('p04_wsum'):
        for m in range(2):
            w_load[m].wait()

            def w_step(i, acc):
                blk = wv[m][:, pl.ds(pl.multiple_of(i * 1024, 1024), 1024)]
                return acc + fold(blk * blk)

            w_acc = lax.fori_loop(0, width // 1024, w_step, jnp.zeros((tile, 128), F32))
            sc_buf[0, 4 * m + 2:4 * m + 3, :] = jnp.sum(w_acc, axis=0, keepdims=True)
        drain(so_buf, sem_in.at[1])
        drain(bo_buf, sem_in.at[2])
        old0 = jnp.sum(so_buf[0], axis=1, keepdims=True) * (0.5 / 128)
        old1 = jnp.sum(bo_buf[1], axis=1, keepdims=True) * (1.0 / (64 * 128))
        sc_buf[0, 3:4, :] = jnp.broadcast_to(old0, (1, 128))
        sc_buf[0, 7:8, :] = jnp.broadcast_to(old1, (1, 128))
        for m in range(2):
            sc_buf[0, 4 * m + 1:4 * m + 2, :] = jnp.sum(rs_own[m], axis=0, keepdims=True)

    hyper_load.wait()
    beta_two = hyper[0]
    rho_step = hyper[1]
    clip_max = hyper[2]
    eye = lax.broadcasted_iota(jnp.int32, (tile, tile), 0) == lax.broadcasted_iota(jnp.int32, (tile, tile), 1)
    for m in range(2):
        with jax.named_scope('p05_rs_wait%d' % m):
            drain(rs_in.at[m, tile:2 * N_BLOCK * tile], rs_rs(m))
        total = rs_own[m, 0:tile]
        for j in range(1, N_BLOCK):
            total = total + rs_in[m, rows_of(j)]
        total_far = rs_in[m, rows_of(N_BLOCK)]
        for j in range(1, N_BLOCK):
            total_far = total_far + rs_in[m, rows_of(N_BLOCK + j)]
        total = jnp.sum(total + total_far, axis=1, keepdims=True)
        old = jnp.sum(jnp.where(eye, jnp.broadcast_to(so_buf[m], (tile, tile)), 0.0), axis=1, keepdims=True)
        new = beta_two * old + (1.0 - beta_two) * (total * (1.0 / n_big) + EPS_ONE)
        rp_all[m, 0:tile] = jnp.broadcast_to(new, (tile, 128))
        r_out[m] = jnp.broadcast_to(new, (tile, 128))
        for j in peers:
            rp_copy(m, j).start()
    send_g((0, 0), (0, 1))

    for m in range(2):
        with jax.named_scope('p07_ar_wait%d' % m):
            drain(ar_buf.at[m, 1:N_BLOCK], ar_rs(m))
        with jax.named_scope('p08_cnew%d' % m):
            total = ar_buf[m, 0]
            for j in range(1, N_BLOCK):
                total = total + ar_buf[m, j]
            old = bo_buf[m, :, pl.ds(base, block)]
            new = beta_two * old + (1.0 - beta_two) * (total * (1.0 / n_small) + EPS_ONE)
            cnew[m] = new
            c_out[m][:, pl.ds(base, block)] = new
        for j in peers:
            c_copy(m, j).start()
        with jax.named_scope('p09_u%d' % m):
            def u_step(i, acc):
                lanes = pl.ds(pl.multiple_of(i * 512, 512), 512)
                blk = gs[m, :, lanes]
                return acc + fold(blk * blk * (1.0 / cnew[m, :, lanes]))

            u_acc = lax.fori_loop(0, block // 512, u_step, jnp.zeros((N_BLOCK * tile, 128), F32))
        with jax.named_scope('p10_rp%d' % m):
            drain(rp_all.at[m, tile:N_BLOCK * tile], rp_rs(m))
        sc_buf[0, 4 * m:4 * m + 1, :] = jnp.sum(u_acc * SCALE / rp_all[m], axis=0, keepdims=True)

    for j in peers:
        sc_copy(j).start()
    send_g((0, 2), (0, 3), (1, 0), (1, 1))
    with jax.named_scope('p11_far'):
        products_far(0)
        products_far(1)
    with jax.named_scope('p11_sc_wait'):
        drain(sc_buf.at[1:N_BLOCK], sc_rs)
        drain(sc_buf.at[1:N_BLOCK], sc_ss)
    total = sc_buf[0]
    for j in peers:
        total = total + sc_buf[j]
    sh_buf[0] = total
    for j in peers:
        sh_copy(j).start()
    for j in peers + (0,):
        sf_copy(j).start()
    send_g((1, 2), (1, 3))
    with jax.named_scope('p12_sh_wait'):
        drain(sh_buf.at[1:2 * N_BLOCK], sh_rs)
    total = sh_buf[0]
    for j in range(1, 2 * N_BLOCK):
        total = total + sh_buf[j]
    sums = jnp.broadcast_to(jnp.sum(total, axis=1, keepdims=True), (8, 128))
    n_total = float(n_small) * float(n_big)
    for m, n_rows in ((0, n_small), (1, n_big)):
        u_sum, g_sum, w_sum, r_sum = (sums[4 * m + i:4 * m + i + 1] for i in range(4))
        row_mean = beta_two * (r_sum * (1.0 / n_rows)) + (1.0 - beta_two) * (g_sum * (1.0 / n_total) + EPS_ONE)
        upd_rms = jnp.sqrt(u_sum * row_mean * (1.0 / (n_total * SCALE)))
        w_rms = jnp.sqrt(w_sum * (1.0 / n_total))
        step_size = rho_step * jnp.maximum(EPS_TWO, w_rms) / jnp.maximum(1.0, upd_rms / clip_max)
        s_out[m:m + 1, :] = step_size * jnp.sqrt(row_mean)

    with jax.named_scope('p13_final'):
        n_link = len(links)
        for m in range(2):
            drain(c_out[m].at[:, 0:(N_BLOCK - 1) * block], c_rs(m))
            drain(g_out[m].at[:, 0:n_link * block], g_rs(m))
        drain(a_all.at[:, tile:N_BLOCK * tile], a_ss)
        drain(rs_in.at[:, tile:2 * N_BLOCK * tile], rs_ss)
        drain(rp_all.at[:, tile:N_BLOCK * tile], rp_ss)
        drain(ar_buf.at[:, 1:N_BLOCK], ar_ss)
        for m in range(2):
            drain(c_out[m].at[:, 0:(N_BLOCK - 1) * block], c_ss)
        drain(gs.at[:, tile:(1 + n_link) * tile], g_ss)
        drain(sh_buf.at[1:2 * N_BLOCK], sh_ss)


def apply_kernel(g0, g1, w0, w1, c0, c1, r_new, scal, w0_new, w1_new, c0_new, c1_new, r0_new, r1_new,
                 w_buf, r_buf, sems):
    tile, width = w0.shape
    step = 4096
    eye = lax.broadcasted_iota(jnp.int32, (tile, tile), 0) == lax.broadcasted_iota(jnp.int32, (tile, tile), 1)
    c_new, r_out, w_new = (c0_new, c1_new), (r0_new, r1_new), (w0_new, w1_new)
    c_old = (c0, c1)
    for m in range(2):
        pltpu.make_async_copy(c_old[m], c_new[m], sems.at[2]).start()
        r_buf[m] = jnp.sum(jnp.where(eye, r_new[m, :, 0:tile], 0.0), axis=0, keepdims=True)
    for m, (g, w, c) in enumerate(((g0, w0, c0), (g1, w1, c1))):
        row_scale = scal[m:m + 1, 0:1] * lax.rsqrt(r_new[m, :, 0:1])
        for i in range(width // step):
            lanes = slice(i * step, (i + 1) * step)
            w_buf[m, :, lanes] = w[:, lanes] - (g[:, lanes] * lax.rsqrt(c[:, lanes])) * row_scale
            pltpu.make_async_copy(w_buf.at[m, :, lanes], w_new[m].at[:, lanes], sems.at[m]).start()
    for m in range(2):
        pltpu.make_async_copy(r_buf.at[m], r_out[m], sems.at[3]).start()
    for m in range(2):
        pltpu.make_async_copy(w_buf.at[m], w_new[m], sems.at[m]).wait()
    for m in range(2):
        pltpu.make_async_copy(c_old[m], c_new[m], sems.at[2]).wait()
    for m in range(2):
        pltpu.make_async_copy(r_buf.at[m], r_out[m], sems.at[3]).wait()


def solution(mesh):
    tile_in = P(None, 'row', 'col')
    tile_out = P(None, 'col', 'row')
    lane_row = P(None, None, 'row')
    lane_col = P(None, None, 'col')
    vec_row = P(None, 'row')
    vec_col = P(None, 'col')
    n_row = mesh.shape['row']
    n_col = mesh.shape['col']

    def local_step(hyper_params, w_in, x_in, dy_in, row_in, col_in, w_out, x_out, dy_out, row_out, col_out):
        tile, width = w_in.shape[1], w_in.shape[2]
        tokens = x_in.shape[1]
        block = width // N_BLOCK
        n_chunk = block // CHUNK
        dims = (tile, width, block, tile * n_row, width * n_col)
        rows = N_BLOCK * tile
        w0 = w_in[0]
        w1 = jnp.transpose(w_out[0])
        a0 = jnp.transpose(x_in[0])
        a1 = jnp.transpose(dy_out[0])
        dma = pltpu.SemaphoreType.DMA
        any_spec = pl.BlockSpec(memory_space=pl.ANY)
        hbm_spec = pl.BlockSpec(memory_space=pltpu.HBM)
        vmem_spec = pl.BlockSpec(memory_space=pltpu.VMEM)
        big = jax.ShapeDtypeStruct((tile, width), F32)
        vec = jax.ShapeDtypeStruct((1, width), F32)
        short = jax.ShapeDtypeStruct((1, tile), F32)
        g0, g1, c0, c1, wv0, wv1, r_new, scal = pl.pallas_call(
            functools.partial(stats_kernel, dims),
            out_shape=(big, big, vec, vec, big, big, jax.ShapeDtypeStruct((2, tile, 128), F32), jax.ShapeDtypeStruct((8, 128), F32)),
            in_specs=[hbm_spec] * 11,
            out_specs=(vmem_spec,) * 8,
            scratch_shapes=[
                pltpu.SMEM((3,), F32),
                pltpu.VMEM((2, rows, tokens), jnp.bfloat16),
                pltpu.VMEM((2, tokens, block), jnp.bfloat16),
                pltpu.VMEM((2, tokens, block), jnp.bfloat16),
                pltpu.VMEM((2, rows, block), F32),
                pltpu.VMEM((2, 1, tile), F32),
                pltpu.VMEM((2, 1, width), F32),
                pltpu.VMEM((2, N_BLOCK, 1, block), F32),
                pltpu.VMEM((2, 1, block), F32),
                pltpu.VMEM((2, rows, 128), F32),
                pltpu.VMEM((2, 2 * rows, 128), F32),
                pltpu.VMEM((2, rows, 128), F32),
                pltpu.VMEM((N_BLOCK, 8, 128), F32),
                pltpu.VMEM((2 * N_BLOCK, 8, 128), F32),
                dma((4,)), dma((2,)), dma((4,)), dma((6, 2)), dma((10,)),
            ],
            compiler_params=pltpu.CompilerParams(collective_id=0, has_side_effects=True, vmem_limit_bytes=40 * 1024 * 1024),
            name='stats',
        )(*[pltpu.with_memory_space_constraint(v, pltpu.HBM) for v in (hyper_params, a0, a1, row_in, col_out, col_in, row_out, dy_in[0], x_out[0], w0, w1)])

        w0_new, w1_new, c0_new, c1_new, r0_new, r1_new = pl.pallas_call(
            apply_kernel,
            out_shape=(big, big, vec, vec, short, short),
            in_specs=[vmem_spec] * 8,
            out_specs=(hbm_spec,) * 6,
            scratch_shapes=[pltpu.VMEM((2, tile, width), F32), pltpu.VMEM((2, 1, tile), F32), dma((4,))],
            compiler_params=pltpu.CompilerParams(vmem_limit_bytes=6 * 1024 * 1024),
            name='apply',
        )(g0, g1, wv0, wv1, c0, c1, r_new, scal)
        return w0_new[None], r0_new, c0_new, jnp.transpose(w1_new)[None], c1_new, r1_new

    return jax.shard_map(local_step, mesh=mesh, in_specs=(P(), tile_in, lane_row, lane_col, vec_row, vec_col, tile_out, lane_col, lane_row, vec_col, vec_row), out_specs=(tile_in, vec_row, vec_col, tile_out, vec_col, vec_row), check_vma=False)
```

```python
import functools

import jax
import jax.numpy as jnp
from jax import lax
from jax.experimental import pallas as pl
from jax.experimental.pallas import tpu as pltpu
from jax.sharding import PartitionSpec as P

EPS_ONE = 1e-30
EPS_TWO = 1e-3
MESH = pl.DeviceIdType.MESH
F32 = jnp.float32

SHARE = ((0, 1, 3, 4, 12, 16, 48, 5), (0, 1, 3, 4, 12, 16, 48, 60))
CODE = (0, 14, 33, 55, 24, 22, 57, 47)
PARTNERS = tuple(sorted({m for lst in SHARE for m in lst[1:]} | {2, 7, 8, 19, 32}))
FAR_PARTNERS = tuple(sorted({m for lst in SHARE for m in lst}))
N_BLOCK = 8
CHUNK = 1024
SCALE = 2.0 ** -20


def digit_xor(v, m):
    if m == 0:
        return v
    if m == 1:
        return v + 1 - 2 * (v % 2)
    if m == 2:
        return (v + 2) % 4
    return 3 - v


def fold(x):
    acc = x[:, 0:128]
    for i in range(1, x.shape[1] // 128):
        acc = acc + x[:, i * 128:(i + 1) * 128]
    return acc


def stats_kernel(dims, hyper_in, a0, a1, so0, so1, bo0, bo1, b0, b1, w0, w1,
                 g0, g1, c0, c1, wv0, wv1, r_out, s_out,
                 hyper, a_all, b_buf, b_far, gs, so_buf, bo_buf, ar_buf, cnew, rs_own, rs_in, rp_all,
                 sc_buf, sh_buf,
                 sem_b, sem_w, sem_in, sem_pair, sem_one):
    tile, width, block, n_small, n_big = dims
    n_chunk = block // CHUNK
    col = lax.axis_index('col')
    row = lax.axis_index('row')
    x, y, z = row % 4, (row // 4) % 4, row // 16
    bx, by, bz = x // 2, y // 2, z // 2
    ax, ay, az = (x + bx) % 2, (y + by) % 2, (z + bz) % 2
    syn = (ax + by + az) % 2 + 2 * ((bx + ay + by) % 2) + 4 * ((ay + az + bz) % 2)
    rank = bx + 2 * bz + 4 * ay
    base = pl.multiple_of(syn * block, block)
    base_far = pl.multiple_of((N_BLOCK - 1 - syn) * block, block)
    peers = (N_BLOCK - 1,) + tuple(range(1, N_BLOCK - 1))
    a_rs, g_rs, rs_rs, rp_rs, c_rs, ar_rs = (lambda m, i=i: sem_pair.at[i, m] for i in range(6))
    a_ss, g_ss, rs_ss, rp_ss, c_ss, ar_ss, sc_ss, sh_ss, sc_rs, sh_rs = (sem_one.at[i] for i in range(10))
    links = range(1, N_BLOCK - 1)

    def peer_row(mask):
        return digit_xor(z, mask // 16) * 16 + digit_xor(y, (mask // 4) % 4) * 4 + digit_xor(x, mask % 4)

    def near(mask):
        return (col, peer_row(mask))

    def far(mask):
        return (1 - col, peer_row(mask))

    a_in, so_in, bo_in, b_in, w_in = (a0, a1), (so0, so1), (bo0, bo1), (b0, b1), (w0, w1)
    g_out, c_out, wv = (g0, g1), (c0, c1), (wv0, wv1)

    def rcopy(src, dst, ss, rs, dev):
        return pltpu.make_async_remote_copy(src_ref=src, dst_ref=dst, send_sem=ss, recv_sem=rs, device_id=dev, device_id_type=MESH)

    barrier = pltpu.get_barrier_semaphore()
    for mask in PARTNERS:
        pl.semaphore_signal(barrier, inc=1, device_id=near(mask), device_id_type=MESH)
    for mask in FAR_PARTNERS:
        pl.semaphore_signal(barrier, inc=1, device_id=far(mask), device_id_type=MESH)

    def drain(ref, sem):
        pltpu.make_async_copy(ref, ref, sem).wait()

    a_load = [pltpu.make_async_copy(a_in[m], a_all.at[m, 0:tile], sem_in.at[0]) for m in range(2)]
    for cp in a_load:
        cp.start()

    def b_load(m, c):
        return pltpu.make_async_copy(b_in[m].at[:, pl.ds(pl.multiple_of(base + c * CHUNK, CHUNK), CHUNK)],
                                     b_buf.at[m, :, c * CHUNK:(c + 1) * CHUNK], sem_b.at[m])

    def b_far_load(m):
        return pltpu.make_async_copy(b_in[m].at[:, pl.ds(base_far, block)], b_far.at[m], sem_b.at[2 + m])

    so_load = [pltpu.make_async_copy(so_in[m], so_buf.at[m], sem_in.at[1]) for m in range(2)]
    bo_load = [pltpu.make_async_copy(bo_in[m], bo_buf.at[m], sem_in.at[2]) for m in range(2)]
    w_load = [pltpu.make_async_copy(w_in[m], wv[m], sem_w.at[m]) for m in range(2)]
    hyper_load = pltpu.make_async_copy(hyper_in, hyper, sem_in.at[3])
    hyper_load.start()
    drain(a_all.at[:, 0:tile], sem_in.at[0])
    for c in range(n_chunk):
        b_load(0, c).start()
    with jax.named_scope('p00_barrier'):
        pl.semaphore_wait(barrier, len(PARTNERS) + len(FAR_PARTNERS))

    def rows_of(j):
        return slice(j * tile, (j + 1) * tile)

    def a_copy(m, j):
        return rcopy(a_all.at[m, 0:tile], a_all.at[m, rows_of(j)], a_ss, a_rs(m), near(SHARE[m][j]))

    for m in range(2):
        for j in peers:
            a_copy(m, j).start()
    for c in range(n_chunk):
        b_load(1, c).start()
    for cp in so_load + bo_load + w_load:
        cp.start()

    def g_copy(m, j, lo, size):
        return rcopy(gs.at[m, rows_of(j), lo:lo + size], g_out[m].at[:, pl.ds(pl.multiple_of(base + lo, CHUNK), size)],
                     g_ss, g_rs(m), near(SHARE[m][j]))

    def send_g(*portions):
        for m, c in portions:
            for j in links:
                g_copy(m, j, c * CHUNK, CHUNK).start()

    def rs_copy(m, j):
        return rcopy(rs_own.at[m, rows_of(j)], rs_in.at[m, rows_of(j)], rs_ss, rs_rs(m), near(SHARE[m][j]))

    def rf_copy(m, j):
        return rcopy(rs_own.at[m, rows_of(j)], rs_in.at[m, rows_of(N_BLOCK + j)], rs_ss, rs_rs(m), far(SHARE[m][j]))

    def ar_copy(m, j):
        return rcopy(ar_buf.at[m, rank], ar_buf.at[m, rank], ar_ss, ar_rs(m), near(CODE[j]))

    def rp_copy(m, j):
        return rcopy(rp_all.at[m, 0:tile], rp_all.at[m, rows_of(j)], rp_ss, rp_rs(m), near(SHARE[m][j]))

    def c_copy(m, j):
        return rcopy(cnew.at[m], c_out[m].at[:, pl.ds(base, block)], c_ss, c_rs(m), near(SHARE[m][j]))

    def sc_copy(j):
        return rcopy(sc_buf.at[0], sc_buf.at[j], sc_ss, sc_rs, near(CODE[j]))

    def sh_copy(j):
        return rcopy(sh_buf.at[0], sh_buf.at[j], sh_ss, sh_rs, near(SHARE[0][j]))

    def sf_copy(j):
        return rcopy(sh_buf.at[0], sh_buf.at[N_BLOCK + j], sh_ss, sh_rs, far(SHARE[0][j]))

    def products(m):
        drain(b_buf.at[m], sem_b.at[m])
        for h in range(n_chunk // 2):
            lanes = slice(2 * h * CHUNK, 2 * (h + 1) * CHUNK)
            g = jnp.dot(a_all[m], b_buf[m, :, lanes], preferred_element_type=F32)
            gs[m, :, lanes] = g
            sq = g * g
            ar_buf[m, rank, :, lanes] = jnp.sum(sq, axis=0, keepdims=True)
            part = fold(sq)
            rs_own[m] = part if h == 0 else rs_own[m] + part

    def products_far(m):
        b_far_load(m).wait()
        g_out[m][:, pl.ds(base_far, block)] = jnp.dot(a_all[m, 0:tile], b_far[m], preferred_element_type=F32)

    def send_sums(m):
        for j in peers:
            rs_copy(m, j).start()
        for j in peers + (0,):
            rf_copy(m, j).start()

    def send_cols(m):
        for j in peers:
            ar_copy(m, j).start()

    with jax.named_scope('p01_a_wait0'):
        drain(a_all.at[0, tile:N_BLOCK * tile], a_rs(0))
    with jax.named_scope('p02_products0'):
        products(0)
    send_sums(0)
    with jax.named_scope('p03_a_wait1'):
        drain(a_all.at[1, tile:N_BLOCK * tile], a_rs(1))
    send_cols(0)
    send_g((0, 0))
    with jax.named_scope('p04_products1'):
        products(1)
    send_sums(1)
    send_cols(1)
    send_g((0, 1))
    for m in range(2):
        b_far_load(m).start()
    for m in range(2):
        g_out[m][:, pl.ds(base, block)] = gs[m, 0:tile]

    with jax.named_scope('p04_wsum'):
        for m in range(2):
            w_load[m].wait()

            def w_step(i, acc):
                blk = wv[m][:, pl.ds(pl.multiple_of(i * 1024, 1024), 1024)]
                return acc + fold(blk * blk)

            w_acc = lax.fori_loop(0, width // 1024, w_step, jnp.zeros((tile, 128), F32))
            sc_buf[0, 4 * m + 2:4 * m + 3, :] = jnp.sum(w_acc, axis=0, keepdims=True)
        drain(so_buf, sem_in.at[1])
        drain(bo_buf, sem_in.at[2])
        old0 = jnp.sum(so_buf[0], axis=1, keepdims=True) * (0.5 / 128)
        old1 = jnp.sum(bo_buf[1], axis=1, keepdims=True) * (1.0 / (64 * 128))
        sc_buf[0, 3:4, :] = jnp.broadcast_to(old0, (1, 128))
        sc_buf[0, 7:8, :] = jnp.broadcast_to(old1, (1, 128))
        for m in range(2):
            sc_buf[0, 4 * m + 1:4 * m + 2, :] = jnp.sum(rs_own[m], axis=0, keepdims=True)

    hyper_load.wait()
    beta_two = hyper[0]
    rho_step = hyper[1]
    clip_max = hyper[2]
    eye = lax.broadcasted_iota(jnp.int32, (tile, tile), 0) == lax.broadcasted_iota(jnp.int32, (tile, tile), 1)
    for m in range(2):
        with jax.named_scope('p05_rs_wait%d' % m):
            drain(rs_in.at[m, tile:2 * N_BLOCK * tile], rs_rs(m))
        total = rs_own[m, 0:tile]
        for j in range(1, N_BLOCK):
            total = total + rs_in[m, rows_of(j)]
        total_far = rs_in[m, rows_of(N_BLOCK)]
        for j in range(1, N_BLOCK):
            total_far = total_far + rs_in[m, rows_of(N_BLOCK + j)]
        total = jnp.sum(total + total_far, axis=1, keepdims=True)
        old = jnp.sum(jnp.where(eye, jnp.broadcast_to(so_buf[m], (tile, tile)), 0.0), axis=1, keepdims=True)
        new = beta_two * old + (1.0 - beta_two) * (total * (1.0 / n_big) + EPS_ONE)
        rp_all[m, 0:tile] = jnp.broadcast_to(new, (tile, 128))
        r_out[m] = jnp.broadcast_to(new, (tile, 128))
        for j in peers:
            rp_copy(m, j).start()
    send_g((0, 2), (0, 3))

    for m in range(2):
        with jax.named_scope('p07_ar_wait%d' % m):
            drain(ar_buf.at[m, 1:N_BLOCK], ar_rs(m))
        with jax.named_scope('p08_cnew%d' % m):
            total = ar_buf[m, 0]
            for j in range(1, N_BLOCK):
                total = total + ar_buf[m, j]
            old = bo_buf[m, :, pl.ds(base, block)]
            new = beta_two * old + (1.0 - beta_two) * (total * (1.0 / n_small) + EPS_ONE)
            cnew[m] = new
            c_out[m][:, pl.ds(base, block)] = new
        for j in peers:
            c_copy(m, j).start()
        with jax.named_scope('p09_u%d' % m):
            def u_step(i, acc):
                lanes = pl.ds(pl.multiple_of(i * 512, 512), 512)
                blk = gs[m, :, lanes]
                return acc + fold(blk * blk * (1.0 / cnew[m, :, lanes]))

            u_acc = lax.fori_loop(0, block // 512, u_step, jnp.zeros((N_BLOCK * tile, 128), F32))
        with jax.named_scope('p10_rp%d' % m):
            drain(rp_all.at[m, tile:N_BLOCK * tile], rp_rs(m))
        sc_buf[0, 4 * m:4 * m + 1, :] = jnp.sum(u_acc * SCALE / rp_all[m], axis=0, keepdims=True)

    for j in peers:
        sc_copy(j).start()
    send_g((1, 0), (1, 1), (1, 2))
    with jax.named_scope('p11_far'):
        products_far(0)
        products_far(1)
    with jax.named_scope('p11_sc_wait'):
        drain(sc_buf.at[1:N_BLOCK], sc_rs)
        drain(sc_buf.at[1:N_BLOCK], sc_ss)
    total = sc_buf[0]
    for j in peers:
        total = total + sc_buf[j]
    sh_buf[0] = total
    for j in peers:
        sh_copy(j).start()
    for j in peers + (0,):
        sf_copy(j).start()
    send_g((1, 3))
    with jax.named_scope('p12_sh_wait'):
        drain(sh_buf.at[1:2 * N_BLOCK], sh_rs)
    total = sh_buf[0]
    for j in range(1, 2 * N_BLOCK):
        total = total + sh_buf[j]
    sums = jnp.broadcast_to(jnp.sum(total, axis=1, keepdims=True), (8, 128))
    n_total = float(n_small) * float(n_big)
    for m, n_rows in ((0, n_small), (1, n_big)):
        u_sum, g_sum, w_sum, r_sum = (sums[4 * m + i:4 * m + i + 1] for i in range(4))
        row_mean = beta_two * (r_sum * (1.0 / n_rows)) + (1.0 - beta_two) * (g_sum * (1.0 / n_total) + EPS_ONE)
        upd_rms = jnp.sqrt(u_sum * row_mean * (1.0 / (n_total * SCALE)))
        w_rms = jnp.sqrt(w_sum * (1.0 / n_total))
        step_size = rho_step * jnp.maximum(EPS_TWO, w_rms) / jnp.maximum(1.0, upd_rms / clip_max)
        s_out[m:m + 1, :] = step_size * jnp.sqrt(row_mean)

    with jax.named_scope('p13_final'):
        n_link = len(links)
        for m in range(2):
            drain(c_out[m].at[:, 0:(N_BLOCK - 1) * block], c_rs(m))
            drain(g_out[m].at[:, 0:n_link * block], g_rs(m))
        drain(a_all.at[:, tile:N_BLOCK * tile], a_ss)
        drain(rs_in.at[:, tile:2 * N_BLOCK * tile], rs_ss)
        drain(rp_all.at[:, tile:N_BLOCK * tile], rp_ss)
        drain(ar_buf.at[:, 1:N_BLOCK], ar_ss)
        for m in range(2):
            drain(c_out[m].at[:, 0:(N_BLOCK - 1) * block], c_ss)
        drain(gs.at[:, tile:(1 + n_link) * tile], g_ss)
        drain(sh_buf.at[1:2 * N_BLOCK], sh_ss)


def apply_kernel(g0, g1, w0, w1, c0, c1, r_new, scal, w0_new, w1_new, c0_new, c1_new, r0_new, r1_new,
                 w_buf, r_buf, sems):
    tile, width = w0.shape
    step = 4096
    eye = lax.broadcasted_iota(jnp.int32, (tile, tile), 0) == lax.broadcasted_iota(jnp.int32, (tile, tile), 1)
    c_new, r_out, w_new = (c0_new, c1_new), (r0_new, r1_new), (w0_new, w1_new)
    c_old = (c0, c1)
    for m in range(2):
        pltpu.make_async_copy(c_old[m], c_new[m], sems.at[2]).start()
        r_buf[m] = jnp.sum(jnp.where(eye, r_new[m, :, 0:tile], 0.0), axis=0, keepdims=True)
    for m, (g, w, c) in enumerate(((g0, w0, c0), (g1, w1, c1))):
        row_scale = scal[m:m + 1, 0:1] * lax.rsqrt(r_new[m, :, 0:1])
        for i in range(width // step):
            lanes = slice(i * step, (i + 1) * step)
            w_buf[m, :, lanes] = w[:, lanes] - (g[:, lanes] * lax.rsqrt(c[:, lanes])) * row_scale
            pltpu.make_async_copy(w_buf.at[m, :, lanes], w_new[m].at[:, lanes], sems.at[m]).start()
    for m in range(2):
        pltpu.make_async_copy(r_buf.at[m], r_out[m], sems.at[3]).start()
    for m in range(2):
        pltpu.make_async_copy(w_buf.at[m], w_new[m], sems.at[m]).wait()
    for m in range(2):
        pltpu.make_async_copy(c_old[m], c_new[m], sems.at[2]).wait()
    for m in range(2):
        pltpu.make_async_copy(r_buf.at[m], r_out[m], sems.at[3]).wait()


def solution(mesh):
    tile_in = P(None, 'row', 'col')
    tile_out = P(None, 'col', 'row')
    lane_row = P(None, None, 'row')
    lane_col = P(None, None, 'col')
    vec_row = P(None, 'row')
    vec_col = P(None, 'col')
    n_row = mesh.shape['row']
    n_col = mesh.shape['col']

    def local_step(hyper_params, w_in, x_in, dy_in, row_in, col_in, w_out, x_out, dy_out, row_out, col_out):
        tile, width = w_in.shape[1], w_in.shape[2]
        tokens = x_in.shape[1]
        block = width // N_BLOCK
        n_chunk = block // CHUNK
        dims = (tile, width, block, tile * n_row, width * n_col)
        rows = N_BLOCK * tile
        w0 = w_in[0]
        w1 = jnp.transpose(w_out[0])
        a0 = jnp.transpose(x_in[0])
        a1 = jnp.transpose(dy_out[0])
        dma = pltpu.SemaphoreType.DMA
        any_spec = pl.BlockSpec(memory_space=pl.ANY)
        hbm_spec = pl.BlockSpec(memory_space=pltpu.HBM)
        vmem_spec = pl.BlockSpec(memory_space=pltpu.VMEM)
        big = jax.ShapeDtypeStruct((tile, width), F32)
        vec = jax.ShapeDtypeStruct((1, width), F32)
        short = jax.ShapeDtypeStruct((1, tile), F32)
        g0, g1, c0, c1, wv0, wv1, r_new, scal = pl.pallas_call(
            functools.partial(stats_kernel, dims),
            out_shape=(big, big, vec, vec, big, big, jax.ShapeDtypeStruct((2, tile, 128), F32), jax.ShapeDtypeStruct((8, 128), F32)),
            in_specs=[hbm_spec] * 11,
            out_specs=(vmem_spec,) * 8,
            scratch_shapes=[
                pltpu.SMEM((3,), F32),
                pltpu.VMEM((2, rows, tokens), jnp.bfloat16),
                pltpu.VMEM((2, tokens, block), jnp.bfloat16),
                pltpu.VMEM((2, tokens, block), jnp.bfloat16),
                pltpu.VMEM((2, rows, block), F32),
                pltpu.VMEM((2, 1, tile), F32),
                pltpu.VMEM((2, 1, width), F32),
                pltpu.VMEM((2, N_BLOCK, 1, block), F32),
                pltpu.VMEM((2, 1, block), F32),
                pltpu.VMEM((2, rows, 128), F32),
                pltpu.VMEM((2, 2 * rows, 128), F32),
                pltpu.VMEM((2, rows, 128), F32),
                pltpu.VMEM((N_BLOCK, 8, 128), F32),
                pltpu.VMEM((2 * N_BLOCK, 8, 128), F32),
                dma((4,)), dma((2,)), dma((4,)), dma((6, 2)), dma((10,)),
            ],
            compiler_params=pltpu.CompilerParams(collective_id=0, has_side_effects=True, vmem_limit_bytes=40 * 1024 * 1024),
            name='stats',
        )(*[pltpu.with_memory_space_constraint(v, pltpu.HBM) for v in (hyper_params, a0, a1, row_in, col_out, col_in, row_out, dy_in[0], x_out[0], w0, w1)])

        w0_new, w1_new, c0_new, c1_new, r0_new, r1_new = pl.pallas_call(
            apply_kernel,
            out_shape=(big, big, vec, vec, short, short),
            in_specs=[vmem_spec] * 8,
            out_specs=(hbm_spec,) * 6,
            scratch_shapes=[pltpu.VMEM((2, tile, width), F32), pltpu.VMEM((2, 1, tile), F32), dma((4,))],
            compiler_params=pltpu.CompilerParams(vmem_limit_bytes=6 * 1024 * 1024),
            name='apply',
        )(g0, g1, wv0, wv1, c0, c1, r_new, scal)
        return w0_new[None], r0_new, c0_new, jnp.transpose(w1_new)[None], c1_new, r1_new

    return jax.shard_map(local_step, mesh=mesh, in_specs=(P(), tile_in, lane_row, lane_col, vec_row, vec_col, tile_out, lane_col, lane_row, vec_col, vec_row), out_specs=(tile_in, vec_row, vec_col, tile_out, vec_col, vec_row), check_vma=False)
```

```python
import functools

import jax
import jax.numpy as jnp
from jax import lax
from jax.experimental import pallas as pl
from jax.experimental.pallas import tpu as pltpu
from jax.sharding import PartitionSpec as P

EPS_ONE = 1e-30
EPS_TWO = 1e-3
MESH = pl.DeviceIdType.MESH
F32 = jnp.float32

SHARE = ((0, 1, 3, 4, 12, 16, 48, 5), (0, 1, 3, 4, 12, 16, 48, 60))
CODE = (0, 14, 33, 55, 24, 22, 57, 47)
PARTNERS = tuple(sorted({m for lst in SHARE for m in lst[1:]} | {2, 7, 8, 19, 32}))
N_BLOCK = 8
CHUNK = 1024
SCALE = 2.0 ** -20


def digit_xor(v, m):
    if m == 0:
        return v
    if m == 1:
        return v + 1 - 2 * (v % 2)
    if m == 2:
        return (v + 2) % 4
    return 3 - v


def fold(x):
    acc = x[:, 0:128]
    for i in range(1, x.shape[1] // 128):
        acc = acc + x[:, i * 128:(i + 1) * 128]
    return acc


def stats_kernel(dims, hyper_in, a0, a1, so0, so1, bo0, bo1, b0, b1, w0, w1,
                 g0, g1, c0, c1, wv0, wv1, r_out, s_out,
                 hyper, a_all, b_buf, b_far, gs, so_buf, bo_buf, ar_buf, cnew, rs_own, rs_in, rp_all,
                 sc_buf, sh_buf,
                 sem_b, sem_w, sem_in, sem_pair, sem_one):
    tile, width, block, n_small, n_big = dims
    n_chunk = block // CHUNK
    col = lax.axis_index('col')
    row = lax.axis_index('row')
    x, y, z = row % 4, (row // 4) % 4, row // 16
    bx, by, bz = x // 2, y // 2, z // 2
    ax, ay, az = (x + bx) % 2, (y + by) % 2, (z + bz) % 2
    syn = (ax + by + az) % 2 + 2 * ((bx + ay + by) % 2) + 4 * ((ay + az + bz) % 2)
    rank = bx + 2 * bz + 4 * ay
    base = pl.multiple_of(syn * block, block)
    base_far = pl.multiple_of((N_BLOCK - 1 - syn) * block, block)
    peers = (N_BLOCK - 1,) + tuple(range(1, N_BLOCK - 1))
    a_rs, g_rs, rs_rs, rp_rs, c_rs, ar_rs = (lambda m, i=i: sem_pair.at[i, m] for i in range(6))
    a_ss, g_ss, rs_ss, rp_ss, c_ss, ar_ss, sc_ss, sh_ss, sc_rs, sh_rs = (sem_one.at[i] for i in range(10))
    links = range(1, N_BLOCK - 1)

    def peer_row(mask):
        return digit_xor(z, mask // 16) * 16 + digit_xor(y, (mask // 4) % 4) * 4 + digit_xor(x, mask % 4)

    def near(mask):
        return (col, peer_row(mask))

    def far(mask):
        return (1 - col, peer_row(mask))

    a_in, so_in, bo_in, b_in, w_in = (a0, a1), (so0, so1), (bo0, bo1), (b0, b1), (w0, w1)
    g_out, c_out, wv = (g0, g1), (c0, c1), (wv0, wv1)

    def rcopy(src, dst, ss, rs, dev):
        return pltpu.make_async_remote_copy(src_ref=src, dst_ref=dst, send_sem=ss, recv_sem=rs, device_id=dev, device_id_type=MESH)

    barrier = pltpu.get_barrier_semaphore()
    for mask in PARTNERS:
        pl.semaphore_signal(barrier, inc=1, device_id=near(mask), device_id_type=MESH)
    pl.semaphore_signal(barrier, inc=1, device_id=far(0), device_id_type=MESH)

    def drain(ref, sem):
        pltpu.make_async_copy(ref, ref, sem).wait()

    a_load = [pltpu.make_async_copy(a_in[m], a_all.at[m, 0:tile], sem_in.at[0]) for m in range(2)]
    for cp in a_load:
        cp.start()

    def b_load(m, c):
        return pltpu.make_async_copy(b_in[m].at[:, pl.ds(pl.multiple_of(base + c * CHUNK, CHUNK), CHUNK)],
                                     b_buf.at[m, :, c * CHUNK:(c + 1) * CHUNK], sem_b.at[m])

    def b_far_load(m):
        return pltpu.make_async_copy(b_in[m].at[:, pl.ds(base_far, block)], b_far.at[m], sem_b.at[2 + m])

    so_load = [pltpu.make_async_copy(so_in[m], so_buf.at[m], sem_in.at[1]) for m in range(2)]
    bo_load = [pltpu.make_async_copy(bo_in[m], bo_buf.at[m], sem_in.at[2]) for m in range(2)]
    w_load = [pltpu.make_async_copy(w_in[m], wv[m], sem_w.at[m]) for m in range(2)]
    hyper_load = pltpu.make_async_copy(hyper_in, hyper, sem_in.at[3])
    hyper_load.start()
    drain(a_all.at[:, 0:tile], sem_in.at[0])
    for c in range(n_chunk):
        b_load(0, c).start()
    with jax.named_scope('p00_barrier'):
        pl.semaphore_wait(barrier, len(PARTNERS) + 1)

    def rows_of(j):
        return slice(j * tile, (j + 1) * tile)

    def a_copy(m, j):
        return rcopy(a_all.at[m, 0:tile], a_all.at[m, rows_of(j)], a_ss, a_rs(m), near(SHARE[m][j]))

    for m in range(2):
        for j in peers:
            a_copy(m, j).start()
    for c in range(n_chunk):
        b_load(1, c).start()
    for cp in so_load + bo_load + w_load:
        cp.start()

    def g_copy(m, j, lo, size):
        return rcopy(gs.at[m, rows_of(j), lo:lo + size], g_out[m].at[:, pl.ds(pl.multiple_of(base + lo, CHUNK), size)],
                     g_ss, g_rs(m), near(SHARE[m][j]))

    def send_g(*portions):
        for m, c in portions:
            for j in links:
                g_copy(m, j, c * CHUNK, CHUNK).start()

    def rs_copy(m, j):
        return rcopy(rs_own.at[m, rows_of(j)], rs_in.at[m, rows_of(j)], rs_ss, rs_rs(m), near(SHARE[m][j]))

    def rf_copy(m, j):
        return rcopy(rs_own.at[m, rows_of(j)], rs_in.at[m, rows_of(N_BLOCK + j)], rs_ss, rs_rs(m), far(SHARE[m][j]))

    def ar_copy(m, j):
        return rcopy(ar_buf.at[m, rank], ar_buf.at[m, rank], ar_ss, ar_rs(m), near(CODE[j]))

    def rp_copy(m, j):
        return rcopy(rp_all.at[m, 0:tile], rp_all.at[m, rows_of(j)], rp_ss, rp_rs(m), near(SHARE[m][j]))

    def c_copy(m, j):
        return rcopy(cnew.at[m], c_out[m].at[:, pl.ds(base, block)], c_ss, c_rs(m), near(SHARE[m][j]))

    def sc_copy(j):
        return rcopy(sc_buf.at[0], sc_buf.at[j], sc_ss, sc_rs, near(CODE[j]))

    def sh_copy(j):
        return rcopy(sh_buf.at[0], sh_buf.at[j], sh_ss, sh_rs, near(SHARE[0][j]))

    def sf_copy(j):
        return rcopy(sh_buf.at[0], sh_buf.at[N_BLOCK + j], sh_ss, sh_rs, far(SHARE[0][j]))

    def products(m):
        drain(b_buf.at[m], sem_b.at[m])
        for h in range(n_chunk // 2):
            lanes = slice(2 * h * CHUNK, 2 * (h + 1) * CHUNK)
            g = jnp.dot(a_all[m], b_buf[m, :, lanes], preferred_element_type=F32)
            gs[m, :, lanes] = g
            sq = g * g
            ar_buf[m, rank, :, lanes] = jnp.sum(sq, axis=0, keepdims=True)
            part = fold(sq)
            rs_own[m] = part if h == 0 else rs_own[m] + part

    def products_far(m):
        b_far_load(m).wait()
        g_out[m][:, pl.ds(base_far, block)] = jnp.dot(a_all[m, 0:tile], b_far[m], preferred_element_type=F32)

    def send_sums(m):
        for j in peers + (0,):
            rf_copy(m, j).start()
        for j in peers:
            rs_copy(m, j).start()

    def send_cols(m):
        for j in peers:
            ar_copy(m, j).start()

    with jax.named_scope('p01_a_wait0'):
        drain(a_all.at[0, tile:N_BLOCK * tile], a_rs(0))
    with jax.named_scope('p02_products0'):
        products(0)
    send_sums(0)
    with jax.named_scope('p03_a_wait1'):
        drain(a_all.at[1, tile:N_BLOCK * tile], a_rs(1))
    send_cols(0)
    with jax.named_scope('p04_products1'):
        products(1)
    send_sums(1)
    send_cols(1)
    for m in range(2):
        b_far_load(m).start()
    for m in range(2):
        g_out[m][:, pl.ds(base, block)] = gs[m, 0:tile]

    with jax.named_scope('p04_wsum'):
        for m in range(2):
            w_load[m].wait()

            def w_step(i, acc):
                blk = wv[m][:, pl.ds(pl.multiple_of(i * 1024, 1024), 1024)]
                return acc + fold(blk * blk)

            w_acc = lax.fori_loop(0, width // 1024, w_step, jnp.zeros((tile, 128), F32))
            sc_buf[0, 4 * m + 2:4 * m + 3, :] = jnp.sum(w_acc, axis=0, keepdims=True)
        drain(so_buf, sem_in.at[1])
        drain(bo_buf, sem_in.at[2])
        old0 = jnp.sum(so_buf[0], axis=1, keepdims=True) * (0.5 / 128)
        old1 = jnp.sum(bo_buf[1], axis=1, keepdims=True) * (1.0 / (64 * 128))
        sc_buf[0, 3:4, :] = jnp.broadcast_to(old0, (1, 128))
        sc_buf[0, 7:8, :] = jnp.broadcast_to(old1, (1, 128))
        for m in range(2):
            sc_buf[0, 4 * m + 1:4 * m + 2, :] = jnp.sum(rs_own[m], axis=0, keepdims=True)

    hyper_load.wait()
    beta_two = hyper[0]
    rho_step = hyper[1]
    clip_max = hyper[2]
    eye = lax.broadcasted_iota(jnp.int32, (tile, tile), 0) == lax.broadcasted_iota(jnp.int32, (tile, tile), 1)
    for m in range(2):
        with jax.named_scope('p05_rs_wait%d' % m):
            drain(rs_in.at[m, tile:2 * N_BLOCK * tile], rs_rs(m))
        total = rs_own[m, 0:tile]
        for j in range(1, N_BLOCK):
            total = total + rs_in[m, rows_of(j)]
        total_far = rs_in[m, rows_of(N_BLOCK)]
        for j in range(1, N_BLOCK):
            total_far = total_far + rs_in[m, rows_of(N_BLOCK + j)]
        total = jnp.sum(total + total_far, axis=1, keepdims=True)
        old = jnp.sum(jnp.where(eye, jnp.broadcast_to(so_buf[m], (tile, tile)), 0.0), axis=1, keepdims=True)
        new = beta_two * old + (1.0 - beta_two) * (total * (1.0 / n_big) + EPS_ONE)
        rp_all[m, 0:tile] = jnp.broadcast_to(new, (tile, 128))
        r_out[m] = jnp.broadcast_to(new, (tile, 128))
        for j in peers:
            rp_copy(m, j).start()
        if m == 0:
            send_g((0, 0))
    send_g((0, 1), (0, 2))

    for m in range(2):
        with jax.named_scope('p07_ar_wait%d' % m):
            drain(ar_buf.at[m, 1:N_BLOCK], ar_rs(m))
        with jax.named_scope('p08_cnew%d' % m):
            total = ar_buf[m, 0]
            for j in range(1, N_BLOCK):
                total = total + ar_buf[m, j]
            old = bo_buf[m, :, pl.ds(base, block)]
            new = beta_two * old + (1.0 - beta_two) * (total * (1.0 / n_small) + EPS_ONE)
            cnew[m] = new
            c_out[m][:, pl.ds(base, block)] = new
        for j in peers:
            c_copy(m, j).start()
        with jax.named_scope('p09_u%d' % m):
            def u_step(i, acc):
                lanes = pl.ds(pl.multiple_of(i * 512, 512), 512)
                blk = gs[m, :, lanes]
                return acc + fold(blk * blk * (1.0 / cnew[m, :, lanes]))

            u_acc = lax.fori_loop(0, block // 512, u_step, jnp.zeros((N_BLOCK * tile, 128), F32))
        with jax.named_scope('p10_rp%d' % m):
            drain(rp_all.at[m, tile:N_BLOCK * tile], rp_rs(m))
        sc_buf[0, 4 * m:4 * m + 1, :] = jnp.sum(u_acc * SCALE / rp_all[m], axis=0, keepdims=True)

    for j in peers:
        sc_copy(j).start()
    send_g((0, 3), (1, 0), (1, 1))
    with jax.named_scope('p11_far'):
        products_far(0)
        products_far(1)
    with jax.named_scope('p11_sc_wait'):
        drain(sc_buf.at[1:N_BLOCK], sc_rs)
        drain(sc_buf.at[1:N_BLOCK], sc_ss)
    total = sc_buf[0]
    for j in peers:
        total = total + sc_buf[j]
    sh_buf[0] = total
    for j in peers + (0,):
        sf_copy(j).start()
    for j in peers:
        sh_copy(j).start()
    send_g((1, 2), (1, 3))
    with jax.named_scope('p12_sh_wait'):
        drain(sh_buf.at[1:2 * N_BLOCK], sh_rs)
    total = sh_buf[0]
    for j in range(1, 2 * N_BLOCK):
        total = total + sh_buf[j]
    sums = jnp.broadcast_to(jnp.sum(total, axis=1, keepdims=True), (8, 128))
    n_total = float(n_small) * float(n_big)
    for m, n_rows in ((0, n_small), (1, n_big)):
        u_sum, g_sum, w_sum, r_sum = (sums[4 * m + i:4 * m + i + 1] for i in range(4))
        row_mean = beta_two * (r_sum * (1.0 / n_rows)) + (1.0 - beta_two) * (g_sum * (1.0 / n_total) + EPS_ONE)
        upd_rms = jnp.sqrt(u_sum * row_mean * (1.0 / (n_total * SCALE)))
        w_rms = jnp.sqrt(w_sum * (1.0 / n_total))
        step_size = rho_step * jnp.maximum(EPS_TWO, w_rms) / jnp.maximum(1.0, upd_rms / clip_max)
        s_out[m:m + 1, :] = step_size * jnp.sqrt(row_mean)

    with jax.named_scope('p13_final'):
        n_link = len(links)
        for m in range(2):
            drain(c_out[m].at[:, 0:(N_BLOCK - 1) * block], c_rs(m))
            drain(g_out[m].at[:, 0:n_link * block], g_rs(m))
        drain(a_all.at[:, tile:N_BLOCK * tile], a_ss)
        drain(rs_in.at[:, tile:2 * N_BLOCK * tile], rs_ss)
        drain(rp_all.at[:, tile:N_BLOCK * tile], rp_ss)
        drain(ar_buf.at[:, 1:N_BLOCK], ar_ss)
        for m in range(2):
            drain(c_out[m].at[:, 0:(N_BLOCK - 1) * block], c_ss)
        drain(gs.at[:, tile:(1 + n_link) * tile], g_ss)
        drain(sh_buf.at[1:2 * N_BLOCK], sh_ss)


def apply_kernel(g0, g1, w0, w1, c0, c1, r_new, scal, w0_new, w1_new, c0_new, c1_new, r0_new, r1_new,
                 w_buf, r_buf, sems):
    tile, width = w0.shape
    step = 4096
    eye = lax.broadcasted_iota(jnp.int32, (tile, tile), 0) == lax.broadcasted_iota(jnp.int32, (tile, tile), 1)
    c_new, r_out, w_new = (c0_new, c1_new), (r0_new, r1_new), (w0_new, w1_new)
    c_old = (c0, c1)
    for m in range(2):
        pltpu.make_async_copy(c_old[m], c_new[m], sems.at[2]).start()
        r_buf[m] = jnp.sum(jnp.where(eye, r_new[m, :, 0:tile], 0.0), axis=0, keepdims=True)
    for m, (g, w, c) in enumerate(((g0, w0, c0), (g1, w1, c1))):
        row_scale = scal[m:m + 1, 0:1] * lax.rsqrt(r_new[m, :, 0:1])
        for i in range(width // step):
            lanes = slice(i * step, (i + 1) * step)
            w_buf[m, :, lanes] = w[:, lanes] - (g[:, lanes] * lax.rsqrt(c[:, lanes])) * row_scale
            pltpu.make_async_copy(w_buf.at[m, :, lanes], w_new[m].at[:, lanes], sems.at[m]).start()
    for m in range(2):
        pltpu.make_async_copy(r_buf.at[m], r_out[m], sems.at[3]).start()
    for m in range(2):
        pltpu.make_async_copy(w_buf.at[m], w_new[m], sems.at[m]).wait()
    for m in range(2):
        pltpu.make_async_copy(c_old[m], c_new[m], sems.at[2]).wait()
    for m in range(2):
        pltpu.make_async_copy(r_buf.at[m], r_out[m], sems.at[3]).wait()


def solution(mesh):
    tile_in = P(None, 'row', 'col')
    tile_out = P(None, 'col', 'row')
    lane_row = P(None, None, 'row')
    lane_col = P(None, None, 'col')
    vec_row = P(None, 'row')
    vec_col = P(None, 'col')
    n_row = mesh.shape['row']
    n_col = mesh.shape['col']

    def local_step(hyper_params, w_in, x_in, dy_in, row_in, col_in, w_out, x_out, dy_out, row_out, col_out):
        tile, width = w_in.shape[1], w_in.shape[2]
        tokens = x_in.shape[1]
        block = width // N_BLOCK
        n_chunk = block // CHUNK
        dims = (tile, width, block, tile * n_row, width * n_col)
        rows = N_BLOCK * tile
        w0 = w_in[0]
        w1 = jnp.transpose(w_out[0])
        a0 = jnp.transpose(x_in[0])
        a1 = jnp.transpose(dy_out[0])
        dma = pltpu.SemaphoreType.DMA
        any_spec = pl.BlockSpec(memory_space=pl.ANY)
        hbm_spec = pl.BlockSpec(memory_space=pltpu.HBM)
        vmem_spec = pl.BlockSpec(memory_space=pltpu.VMEM)
        big = jax.ShapeDtypeStruct((tile, width), F32)
        vec = jax.ShapeDtypeStruct((1, width), F32)
        short = jax.ShapeDtypeStruct((1, tile), F32)
        g0, g1, c0, c1, wv0, wv1, r_new, scal = pl.pallas_call(
            functools.partial(stats_kernel, dims),
            out_shape=(big, big, vec, vec, big, big, jax.ShapeDtypeStruct((2, tile, 128), F32), jax.ShapeDtypeStruct((8, 128), F32)),
            in_specs=[hbm_spec] * 11,
            out_specs=(vmem_spec,) * 8,
            scratch_shapes=[
                pltpu.SMEM((3,), F32),
                pltpu.VMEM((2, rows, tokens), jnp.bfloat16),
                pltpu.VMEM((2, tokens, block), jnp.bfloat16),
                pltpu.VMEM((2, tokens, block), jnp.bfloat16),
                pltpu.VMEM((2, rows, block), F32),
                pltpu.VMEM((2, 1, tile), F32),
                pltpu.VMEM((2, 1, width), F32),
                pltpu.VMEM((2, N_BLOCK, 1, block), F32),
                pltpu.VMEM((2, 1, block), F32),
                pltpu.VMEM((2, rows, 128), F32),
                pltpu.VMEM((2, 2 * rows, 128), F32),
                pltpu.VMEM((2, rows, 128), F32),
                pltpu.VMEM((N_BLOCK, 8, 128), F32),
                pltpu.VMEM((2 * N_BLOCK, 8, 128), F32),
                dma((4,)), dma((2,)), dma((4,)), dma((6, 2)), dma((10,)),
            ],
            compiler_params=pltpu.CompilerParams(collective_id=0, has_side_effects=True, vmem_limit_bytes=40 * 1024 * 1024),
            name='stats',
        )(*[pltpu.with_memory_space_constraint(v, pltpu.HBM) for v in (hyper_params, a0, a1, row_in, col_out, col_in, row_out, dy_in[0], x_out[0], w0, w1)])

        w0_new, w1_new, c0_new, c1_new, r0_new, r1_new = pl.pallas_call(
            apply_kernel,
            out_shape=(big, big, vec, vec, short, short),
            in_specs=[vmem_spec] * 8,
            out_specs=(hbm_spec,) * 6,
            scratch_shapes=[pltpu.VMEM((2, tile, width), F32), pltpu.VMEM((2, 1, tile), F32), dma((4,))],
            compiler_params=pltpu.CompilerParams(vmem_limit_bytes=6 * 1024 * 1024),
            name='apply',
        )(g0, g1, wv0, wv1, c0, c1, r_new, scal)
        return w0_new[None], r0_new, c0_new, jnp.transpose(w1_new)[None], c1_new, r1_new

    return jax.shard_map(local_step, mesh=mesh, in_specs=(P(), tile_in, lane_row, lane_col, vec_row, vec_col, tile_out, lane_col, lane_row, vec_col, vec_row), out_specs=(tile_in, vec_row, vec_col, tile_out, vec_col, vec_row), check_vma=False)
```
